256 devices in a mesh: dev: 64 (over z, x, core), rep: 4 (over y).
Axes of the slice: x: 4, y: 4, z: 8, core: 2. Of those that a mesh axis runs over, the one named last changes fastest.
Arguments:
- h_zero: bfloat16 [262144, 256], P(('dev', 'rep')), may hold values from 0 to 2
- h_prev: bfloat16 [262144, 256], P(('dev', 'rep')), may hold values from 0 to 2
- hist_a: bfloat16 [262144, 256], P('dev'), may hold values from 0 to 2
- hist_b: bfloat16 [262144, 256], P('dev'), may hold values from 0 to 2
- tile_vals: bfloat16 [2048, 12, 128, 128], P(('dev', 'rep'))
- tile_cols: int32 [2048, 12], P(('dev', 'rep')), may hold values from 0 to 103, as said below
- pull_rows: int32 [256, 64, 128], P(('dev', 'rep')), may hold values from 0 to 4095
- pull_counts: int32 [256, 64], P(('dev', 'rep')), may hold values from 96 to 128, as said below
- weight_two: bfloat16 [256, 256], replicated, may hold values from -0.375 to 0.375
- weight_three: bfloat16 [256, 256], replicated, may hold values from -0.375 to 0.375
- grad_out: bfloat16 [262144, 256], P(('dev', 'rep')), may hold values from -0.046875 to 0.046875
Outputs:
- layer_three: bfloat16 [262144, 256], P(('dev', 'rep'))
- new_history: bfloat16 [262144, 256], P('dev')
- weight_grad: float32 [256, 256], replicated
The draws below stay inside these ranges and needn't reach their ends.
Inputs may be any that keep to these rules, and one draw needn't show every extreme that they name: `tile_cols`: entry 0 of a row block names one of its device's own 8 blocks; entries 1 to 3 name blocks of the owner's history shard; the other 8 name pulled blocks of consecutive owners modulo 64, and every owner's block is named by some row block of each device. `pull_rows`: entries at slots at or past the block's count are read by no output. `pull_counts`: every device pulls a full block of 128 rows from some owner and a block of exactly 96 rows from another.
All inputs are finite; a program needn't handle non-finite values.
Results may differ from the reference program's by a relative error of at most 0.0034.
Values may be sent and summed in bfloat16 or wider, within the bound.
A program may use at most 128 MiB of HBM per device.

```python
import math
import jax
import jax.numpy as jnp
from jax import lax

WIDTH = 256
BATCH = 1024
TILE = 128
HOME_TILES = 3
REMOTE_TILES = 8
TPR = 12
ROWBLK = 8
WORKERS = 256
SHARD = 4096
NODES = 262144
N_DEV = 64
N_REP = 4


def draw_tile_vals(key, part):
    full_shape = (WORKERS * ROWBLK, TPR, TILE, TILE)
    key_mask, key_value = jax.random.split(key, 2)
    edge_mask = jax.random.bernoulli(key_mask, 0.125, full_shape).astype(jnp.float32)
    edge_weight = jax.random.uniform(key_value, full_shape, jnp.float32, 0.5, 1.5)
    return (edge_mask * edge_weight * (8.0 / (TPR * TILE))).astype(jnp.bfloat16)


def draw_tile_cols(key, part):
    key_local, key_home, key_shift = jax.random.split(key, 3)
    row_count = WORKERS * ROWBLK
    local_cols = jax.random.randint(key_local, (row_count, 1), 0, ROWBLK, jnp.int32)
    home_cols = jax.random.randint(key_home, (row_count, HOME_TILES), ROWBLK, ROWBLK + N_REP * ROWBLK, jnp.int32)
    shifts = jax.random.randint(key_shift, (WORKERS, 1), 0, N_DEV, jnp.int32)
    shift_rows = jnp.repeat(shifts, ROWBLK, axis=0)
    block_pos = (jnp.arange(row_count, dtype=jnp.int32) % ROWBLK)[:, None]
    slot_pos = jnp.arange(REMOTE_TILES, dtype=jnp.int32)[None, :]
    peer_ids = (block_pos * REMOTE_TILES + slot_pos + shift_rows) % N_DEV
    remote_cols = ROWBLK + N_REP * ROWBLK + peer_ids
    return jnp.concatenate([local_cols, home_cols, remote_cols], axis=1).astype(jnp.int32)


def draw_pull_counts(key, part):
    key_one, key_two, key_full = jax.random.split(key, 3)
    full_shape = (WORKERS, N_DEV)
    first = jax.random.randint(key_one, full_shape, 1, TILE + 1, jnp.int32)
    second = jax.random.randint(key_two, full_shape, 1, TILE + 1, jnp.int32)
    counts = TILE - first * second // (4 * TILE)
    offset = jax.random.randint(key_full, (), 0, N_DEV, jnp.int32)
    full_peer = (jnp.arange(WORKERS, dtype=jnp.int32) * 5 + offset) % N_DEV
    low_peer = (full_peer + 1) % N_DEV
    peer_ids = jnp.arange(N_DEV, dtype=jnp.int32)[None, :]
    counts = jnp.where(peer_ids == low_peer[:, None], TILE - TILE // 4, counts)
    counts = jnp.where(peer_ids == full_peer[:, None], TILE, counts)
    return counts.astype(jnp.int32)


def set_ends(drawn, stream_key, low, top_value):
    spot = [jax.random.randint(jax.random.fold_in(stream_key, axis), (), 0, length) for axis, length in enumerate(drawn.shape)]
    longest = drawn.shape.index(max(drawn.shape))
    next_to = spot[:longest] + [(spot[longest] + 1) % drawn.shape[longest]] + spot[longest + 1:]
    return drawn.at[tuple(spot)].set(low).at[tuple(next_to)].set(top_value)


def levels(rng, dims, cuts, low, top_value):
    gain = 1.0
    for axis_at, parts in cuts:
        draws = jax.random.uniform(jax.random.fold_in(jax.random.fold_in(rng, 6), axis_at), (parts,), jnp.float32, low / len(cuts), top_value / len(cuts))
        gain = gain * jnp.repeat(jnp.exp(draws), dims[axis_at] // parts).reshape((-1,) + (1,) * (len(dims) - 1 - axis_at))
    return gain


def gaussian(key, extent, spread, most, pieces=(), kind=jnp.bfloat16):
    level = levels(key, extent, pieces, -0.22, 0.18) if pieces else 1.0
    entries = jax.random.normal(key, extent, jnp.float32) * spread * level
    return jnp.minimum(jnp.maximum(entries, -most), most).astype(kind)


def setup_inputs(seed: int = 0) -> dict:
    key_list = jax.random.split(jax.random.key(seed), 12)
    return {
        "h_zero": jnp.clip(2.0 * jax.random.uniform(key_list[0], (NODES, WIDTH), jnp.float32) ** levels(key_list[0], (NODES, WIDTH), ((0, 256),), -0.2, 0.2), 0.0, 2.0).astype(jnp.bfloat16),
        "h_prev": jnp.clip(2.0 * jax.random.uniform(key_list[1], (NODES, WIDTH), jnp.float32) ** levels(key_list[1], (NODES, WIDTH), ((0, 256),), -0.2, 0.2), 0.0, 2.0).astype(jnp.bfloat16),
        "hist_a": jnp.clip(2.0 * jax.random.uniform(key_list[2], (NODES, WIDTH), jnp.float32) ** levels(key_list[2], (NODES, WIDTH), ((0, 64),), -0.2, 0.2), 0.0, 2.0).astype(jnp.bfloat16),
        "hist_b": jnp.clip(2.0 * jax.random.uniform(key_list[3], (NODES, WIDTH), jnp.float32) ** levels(key_list[3], (NODES, WIDTH), ((0, 64),), -0.2, 0.2), 0.0, 2.0).astype(jnp.bfloat16),
        "tile_vals": draw_tile_vals(jax.random.fold_in(key_list[11], 71), 0),
        "tile_cols": draw_tile_cols(jax.random.fold_in(key_list[11], 71), 0),
        "pull_rows": set_ends(jax.random.randint(key_list[6], (WORKERS, N_DEV, TILE), 0, SHARD), jax.random.fold_in(key_list[6], 1), 0, SHARD - 1).astype(jnp.int32),
        "pull_counts": draw_pull_counts(jax.random.fold_in(key_list[11], 71), 0),
        "weight_two": gaussian(key_list[8], (WIDTH, WIDTH), WIDTH ** -0.5, 0.375),
        "weight_three": gaussian(key_list[9], (WIDTH, WIDTH), WIDTH ** -0.5, 0.375),
        "grad_out": gaussian(key_list[10], (NODES, WIDTH), (4.0 / NODES ** 0.5), 0.046875, ((0, 256),)),
    }


restart = 0.1
strength = 0.5


def propagate(current, history, pulled, values, columns, start_rows, weight, layer_number):
    feature_width = current.shape[1]
    source = jnp.concatenate([current, history, pulled.reshape(-1, feature_width)], axis=0)
    blocks = source.reshape(-1, TILE, feature_width)
    picked = jnp.take(blocks, columns.reshape(-1), axis=0).reshape(columns.shape + (TILE, feature_width))
    summed = jnp.einsum("btij,btjf->bif", values.astype(jnp.float32), picked.astype(jnp.float32))
    summed = summed.reshape(current.shape[0], feature_width)
    mixed_rows = (1.0 - restart) * summed + restart * start_rows.astype(jnp.float32)
    mixed_low = mixed_rows.astype(jnp.bfloat16)
    factor = math.log(strength / layer_number + 1.0)
    product = jnp.dot(mixed_low, weight, preferred_element_type=jnp.float32)
    inner_sum = (1.0 - factor) * mixed_rows + factor * product
    return jnp.maximum(inner_sum, 0.0).astype(jnp.bfloat16), mixed_low


def reference(h_zero, h_prev, hist_a, hist_b, tile_vals, tile_cols, pull_rows, pull_counts, weight_two, weight_three, grad_out):
    shard_a = hist_a.reshape(N_DEV, SHARD, WIDTH)
    shard_b = hist_b.reshape(N_DEV, SHARD, WIDTH)
    owners = jnp.arange(N_DEV, dtype=jnp.int32)[:, None]
    slot_ids = jnp.arange(TILE, dtype=jnp.int32)[None, :]

    def device(items):
        worker, start_rows, current, values, columns, wanted, counts, upstream = items
        home_shard = (worker // N_REP).astype(jnp.int32)
        live_mask = (slot_ids < counts[:, None])[:, :, None]
        pulled_a = jnp.where(live_mask, shard_a[owners, wanted], jnp.zeros((), shard_a.dtype))
        pulled_b = jnp.where(live_mask, shard_b[owners, wanted], jnp.zeros((), shard_b.dtype))
        own_a = lax.dynamic_index_in_dim(shard_a, home_shard, 0, keepdims=False)
        own_b = lax.dynamic_index_in_dim(shard_b, home_shard, 0, keepdims=False)
        second, unused_mix = propagate(current, own_a, pulled_a, values, columns, start_rows, weight_two, 2)
        layer_out, mixed_low = propagate(second, own_b, pulled_b, values, columns, start_rows, weight_three, 3)
        factor = math.log(strength / 3 + 1.0)
        grad_term = factor * jnp.dot(mixed_low.T, upstream, preferred_element_type=jnp.float32)
        return layer_out, second, grad_term

    items = (
        jnp.arange(WORKERS, dtype=jnp.int32),
        h_zero.reshape(WORKERS, BATCH, WIDTH),
        h_prev.reshape(WORKERS, BATCH, WIDTH),
        tile_vals.reshape(WORKERS, ROWBLK, TPR, TILE, TILE),
        tile_cols.reshape(WORKERS, ROWBLK, TPR),
        pull_rows,
        pull_counts,
        grad_out.reshape(WORKERS, BATCH, WIDTH),
    )
    layer_out, second, grad_terms = lax.map(device, items)
    return layer_out.reshape(NODES, WIDTH), second.reshape(NODES, WIDTH), jnp.sum(grad_terms, axis=0)
```

```python
import functools
import math

import jax
import jax.numpy as jnp
from jax import lax
from jax.experimental import pallas as pl
from jax.experimental.pallas import tpu as pltpu
from jax.sharding import Mesh
from jax.sharding import PartitionSpec as P

Z, X, C, Y = "dev_0", "dev_1", "dev_2", "rep"
DEV = (Z, X, C)
DEV_REP = (Z, X, C, Y)
MIB = 1024 * 1024

restart = 0.1
strength = 0.5
BF = jnp.bfloat16
F32 = jnp.float32
VMEM = pltpu.VMEM
SMEM = pltpu.SMEM


def vspec():
    return pl.BlockSpec(memory_space=VMEM)


def sspec():
    return pl.BlockSpec(memory_space=SMEM)


def aspec():
    return pl.BlockSpec(memory_space=pl.ANY)


def cost(flops, nbytes):
    return pl.CostEstimate(flops=int(flops), bytes_accessed=int(nbytes), transcendentals=0)


def pack_kernel(inv_ref, cnt_ref, tiles_ref, extra_ref, out_ref, sem):
    groups = out_ref.shape[0]
    for g in range(groups):
        for d in range(4):
            t = inv_ref[g * 4 + d]
            pltpu.make_async_copy(
                tiles_ref.at[t], out_ref.at[g, pl.ds(0, 128), pl.ds(d * 128, 128)], sem.at[g]
            ).start()
    lane = lax.broadcasted_iota(jnp.int32, (128, 128), 1)

    def one(g, carry):
        for d in range(4):
            pltpu.make_async_copy(
                tiles_ref.at[0], out_ref.at[g, pl.ds(0, 128), pl.ds(d * 128, 128)], sem.at[g]
            ).wait()
        for d in range(4):
            here = (pl.ds(0, 128), pl.ds(d * 128, 128))
            tile = out_ref[g, here[0], here[1]].astype(F32)
            tile = jnp.where(lane < cnt_ref[g * 4 + d], tile, 0.0)
            out_ref[g, here[0], here[1]] = tile.astype(BF)
        out_ref[g, 128:144, :] = extra_ref[g]
        return carry

    lax.fori_loop(0, groups, one, 0)


def packed_tiles(inv, cnt, tiles, extra):
    return pl.pallas_call(
        pack_kernel,
        out_shape=jax.ShapeDtypeStruct((16, 144, 512), BF),
        in_specs=[sspec(), sspec(), aspec(), vspec()],
        out_specs=vspec(),
        scratch_shapes=[pltpu.SemaphoreType.DMA((16,))],
        compiler_params=pltpu.CompilerParams(vmem_limit_bytes=16 * MIB),
        cost_estimate=cost(3e9, 5e6),
    )(inv, cnt, tiles, extra)


def pull_kernel(idx_ref, at_ref, v_ref, own_ref, *refs):
    far = refs[:12]
    same_ref, other_ref, stage, table, got, sem = refs[12:]
    turn, core = at_ref[0], at_ref[1]

    def copies(d):
        for q in range(4):
            if d == 0:
                start = pl.multiple_of(lax.rem(turn + q, 4) * 1024, 1024)
                src = own_ref.at[pl.ds(start, 1024), :]
            else:
                src = far[(d - 1) * 4 + q]
            yield pltpu.make_async_copy(src, stage.at[d, pl.ds(q * 1024, 1024), :], sem.at[d])

    for d in range(4):
        for copy in copies(d):
            copy.start()
    for d in range(4):
        for copy in copies(d):
            copy.wait()

        def widen(s, carry):
            r = pl.multiple_of(s * 128, 128)
            rows = stage[d, pl.ds(r, 128), :].astype(F32)
            table[d, pl.ds(2 * r, 128, stride=2), :] = rows[:, :128]
            table[d, pl.ds(2 * r + 1, 128, stride=2), :] = rows[:, 128:]
            return carry

        lax.fori_loop(0, 32, widen, 0)

    def serve(z, which, out):
        g = z * 2 + which
        for d in range(4):
            for j in range(128):
                i = idx_ref[g * 4 + d, j]
                got[pl.ds(2 * (d * 128 + j), 2), :] = table[d, pl.ds(2 * i, 2), :]
        low, high = got[pl.ds(0, 512, stride=2), :], got[pl.ds(1, 512, stride=2), :]
        rows = jnp.concatenate([low, high], axis=1).astype(BF)
        tiles = v_ref[g, 0:128, :]
        flag = v_ref[g, 130:131, :]
        both = jnp.concatenate([tiles * flag, tiles * (1 - flag)], axis=0)
        out[z] = jnp.dot(both, rows, preferred_element_type=F32).astype(out.dtype)

    def one(z, carry):
        serve(z, 1 - core, other_ref)
        return carry

    def two(z, carry):
        serve(z, core, same_ref)
        return carry

    lax.fori_loop(0, 8, one, 0)
    lax.fori_loop(0, 8, two, 0)


def pulled_sums(idx, at, tiles, own, far):
    return pl.pallas_call(
        pull_kernel,
        out_shape=(
            jax.ShapeDtypeStruct((8, 256, 256), F32),
            jax.ShapeDtypeStruct((8, 256, 256), BF),
        ),
        in_specs=[sspec(), sspec(), vspec()] + [aspec()] * 13,
        out_specs=(vspec(), vspec()),
        scratch_shapes=[
            VMEM((4, 4096, 256), BF),
            VMEM((4, 8192, 128), F32),
            VMEM((1024, 128), F32),
            pltpu.SemaphoreType.DMA((4,)),
        ],
        compiler_params=pltpu.CompilerParams(vmem_limit_bytes=48 * MIB),
        cost_estimate=cost(20e9, 20e6),
    )(idx, at, tiles, own, *far)


def home_kernel(first, cols_ref, tiles_ref, cur_ref, hist_ref, out_ref):
    for i in range(8):
        total = None
        for t in range(first, 4):
            b = cols_ref[i, t]
            if t == 0:
                block = cur_ref[pl.ds(pl.multiple_of(b * 128, 128), 128), :]
            else:
                block = hist_ref[pl.ds(pl.multiple_of((b - 8) * 128, 128), 128), :]
            part = jnp.dot(tiles_ref[i, t], block, preferred_element_type=F32)
            total = part if total is None else total + part
        out_ref[i] = total


def home_sums(first, cols, tiles, cur, hist):
    return pl.pallas_call(
        functools.partial(home_kernel, first),
        grid=(1,),
        out_shape=jax.ShapeDtypeStruct((8, 128, 256), F32),
        in_specs=[
            sspec(),
            pl.BlockSpec((8, 4, 128, 128), lambda i: (0, 0, 0, 0)),
            pl.BlockSpec((1024, 256), lambda i: (0, 0)),
            pl.BlockSpec((4096, 256), lambda i: (0, 0)),
        ],
        out_specs=pl.BlockSpec((8, 128, 256), lambda i: (0, 0, 0)),
        compiler_params=pltpu.CompilerParams(vmem_limit_bytes=24 * MIB),
        cost_estimate=cost(3e9, 5e6),
    )(cols, tiles, cur, hist)


def gathered(total, at_ref, arrived_ref):
    for k in range(8):
        for s in range(2):
            i = at_ref[k, s]
            total[i] = total[i] + arrived_ref[k, pl.ds(s * 128, 128), :].astype(F32)


def layer_two_kernel(at_ref, home_ref, arrived_ref, zero_ref, weight_ref, out_ref, total):
    total[...] = home_ref[...]
    gathered(total, at_ref, arrived_ref)
    factor = math.log(strength / 2 + 1.0)
    mixed = (1.0 - restart) * total[...].reshape(1024, 256) + restart * zero_ref[...].astype(F32)
    product = jnp.dot(mixed.astype(BF), weight_ref[...], preferred_element_type=F32)
    out_ref[...] = jnp.maximum((1.0 - factor) * mixed + factor * product, 0.0).astype(BF)


def layer_two(at, home, arrived, zero, weight):
    return pl.pallas_call(
        layer_two_kernel,
        out_shape=jax.ShapeDtypeStruct((1024, 256), BF),
        in_specs=[sspec()] + [vspec()] * 4,
        out_specs=vspec(),
        scratch_shapes=[VMEM((8, 128, 256), F32)],
        compiler_params=pltpu.CompilerParams(vmem_limit_bytes=24 * MIB),
        cost_estimate=cost(1e9, 4e6),
    )(at, home, arrived, zero, weight)


def layer_three_kernel(
    at_ref, cols_ref, home_ref, arrived_ref, tiles_ref, cur_ref, zero_ref, weight_ref, grad_ref,
    out_ref, term_ref, total,
):
    for i in range(8):
        block = cur_ref[pl.ds(pl.multiple_of(cols_ref[i, 0] * 128, 128), 128), :]
        total[i] = home_ref[i] + jnp.dot(tiles_ref[i, 0], block, preferred_element_type=F32)
    gathered(total, at_ref, arrived_ref)
    factor = math.log(strength / 3 + 1.0)
    mixed = (1.0 - restart) * total[...].reshape(1024, 256) + restart * zero_ref[...].astype(F32)
    low = mixed.astype(BF)
    product = jnp.dot(low, weight_ref[...], preferred_element_type=F32)
    out_ref[...] = jnp.maximum((1.0 - factor) * mixed + factor * product, 0.0).astype(BF)
    term_ref[...] = factor * lax.dot_general(
        low, grad_ref[...], (((0,), (0,)), ((), ())), preferred_element_type=F32
    )


def layer_three_call(at, cols, home, arrived, tiles, cur, zero, weight, grad):
    whole = lambda *shape: pl.BlockSpec(shape, lambda i: (0,) * len(shape))
    return pl.pallas_call(
        layer_three_kernel,
        grid=(1,),
        out_shape=(
            jax.ShapeDtypeStruct((1024, 256), BF),
            jax.ShapeDtypeStruct((256, 256), F32),
        ),
        in_specs=[
            sspec(), sspec(), whole(8, 128, 256), whole(8, 256, 256), whole(8, 1, 128, 128),
            whole(1024, 256), whole(1024, 256), whole(256, 256), whole(1024, 256),
        ],
        out_specs=(whole(1024, 256), whole(256, 256)),
        scratch_shapes=[VMEM((8, 128, 256), F32)],
        compiler_params=pltpu.CompilerParams(vmem_limit_bytes=32 * MIB),
        cost_estimate=cost(1e9, 4e6),
    )(at, cols, home, arrived, tiles, cur, zero, weight, grad)


def in_order(blocks, dim):
    shape = list(blocks.shape[1:])
    shape[dim] *= blocks.shape[0]
    return jnp.moveaxis(blocks, 0, dim).reshape(shape)


def sent_to_all(value, axis):
    copies = jnp.broadcast_to(value, (lax.axis_size(axis), *value.shape))
    return lax.all_to_all(copies, axis, split_axis=0, concat_axis=0, tiled=True)


def gathered_by_axis(value, axes, dim):
    far, near = axes
    initial = sent_to_all(value, far)
    blocks = jnp.swapaxes(sent_to_all(initial, near), 0, 1)
    return in_order(blocks.reshape(-1, *value.shape), dim)


def cut_along(value, dim, length):
    shape = value.shape
    blocks = value.reshape(*shape[:dim], length, shape[dim] // length, *shape[dim + 1 :])
    return jnp.moveaxis(blocks, dim, 0)


def summed_on_arrival(value, axis, dim):
    length = lax.axis_size(axis)
    blocks = lax.all_to_all(cut_along(value, dim, length), axis, 0, 0, tiled=True)
    return jnp.sum(blocks, axis=0)


def summed_rows(value, axes, dim):
    far, near = axes
    blocks = cut_along(value, dim, lax.axis_size(far))
    nearer = summed_on_arrival(blocks, near, dim + 1)
    arrived = lax.all_to_all(nearer, far, split_axis=0, concat_axis=0, tiled=True)
    return arrived.sum(axis=0)


def nested_sum(value, axes):
    return gathered_by_axis(summed_rows(value, axes, 0), axes, 0)


def shifted(value, axis, by):
    n = lax.axis_size(axis)
    return lax.ppermute(value, axis, [((i + by) % n, i) for i in range(n)])


def local(
    h_zero, h_prev, hist_a, hist_b, tile_vals, tile_cols, pull_rows, pull_counts,
    weight_two, weight_three, grad_out,
):
    x, core, turn = lax.axis_index(X), lax.axis_index(C), lax.axis_index(Y)

    def shard(history):
        quarters = history.reshape(4, 1024, 256)
        mine = [
            lax.dynamic_index_in_dim(quarters, lax.rem(turn + q, 4), 0, keepdims=False)
            for q in range(2)
        ]
        far = []
        for d in (1, 3, 2):
            a, b = [shifted(m, X, d) for m in mine]
            far.append((d, [a, b, shifted(b, Y, 1), shifted(a, Y, 3)]))
        return [piece for _, pieces in sorted(far, key=lambda f: f[0]) for piece in pieces]

    far_a = shard(hist_a)
    k = lax.broadcasted_iota(jnp.int32, (8, 2, 4), 0)
    c = lax.broadcasted_iota(jnp.int32, (8, 2, 4), 1)
    d = lax.broadcasted_iota(jnp.int32, (8, 2, 4), 2)
    owner = (8 * k + 2 * lax.rem(x + d, 4) + c).reshape(64)
    named = tile_cols[:, 4:].reshape(64) - 40
    block = lax.broadcasted_iota(jnp.int32, (8, 8), 0).reshape(64)
    place = (lax.broadcasted_iota(jnp.int32, (8, 8), 1) + 12 * block.reshape(8, 8) + 4).reshape(64)
    is_it = named[None, :] == jnp.arange(64, dtype=jnp.int32)[:, None]
    tile_of = jnp.sum(jnp.where(is_it, place[None, :], 0), axis=1)
    block_of = jnp.sum(jnp.where(is_it, block[None, :], 0), axis=1).reshape(8, 8)
    ends = jnp.stack([block_of[:, 0], block_of[:, 7]], axis=1)
    first = (block_of == ends[:, :1]).reshape(64)
    inv = jnp.take(tile_of, owner)
    cnt = jnp.take(pull_counts[0], owner)
    rows = lax.rem(jnp.take(pull_rows[0], owner, axis=0) + (4096 - 1024 * turn), 4096)
    flag = jnp.broadcast_to(jnp.take(first, owner)[:, None], (64, 128))
    extra = jnp.stack([rows // 64, lax.rem(rows, 64), flag.astype(jnp.int32)], axis=1)
    extra = extra.reshape(16, 4, 3, 128).transpose(0, 2, 1, 3).reshape(16, 3, 512)
    extra = jnp.pad(extra.astype(BF), ((0, 0), (0, 13), (0, 0)))
    tiles = packed_tiles(inv, cnt, tile_vals.reshape(96, 128, 128), extra)
    tiles = lax.all_to_all(tiles, (Z, C), split_axis=0, concat_axis=0, tiled=True)
    digits = tiles[:, 128:130, :].astype(F32).astype(jnp.int32)
    idx = (digits[:, 0] * 64 + digits[:, 1]).reshape(64, 128)
    at = jnp.stack([turn, core])

    far_b = shard(hist_b)
    home_a = home_sums(0, tile_cols, tile_vals, h_prev, hist_a)
    home_b = home_sums(1, tile_cols, tile_vals, h_prev, hist_b)

    def arrived_sums(history, far):
        same, other = pulled_sums(idx, at, tiles, history, far)
        out = (same + shifted(other, C, 1).astype(F32)).astype(BF)
        return lax.all_to_all(out, Z, split_axis=0, concat_axis=0, tiled=True)

    arrived_a = arrived_sums(hist_a, far_a)
    second = layer_two(ends, home_a, arrived_a, h_zero, weight_two)
    fresh_rows = in_order(sent_to_all(second, Y), 0)
    arrived_b = arrived_sums(hist_b, far_b)
    layer_three, term = layer_three_call(
        ends, tile_cols, home_b, arrived_b, tile_vals, second, h_zero, weight_three, grad_out
    )
    grad_total = nested_sum(term, ((Z, X), (C, Y)))
    return (layer_three, fresh_rows, grad_total)


def solution(mesh):
    finer = Mesh(mesh.devices.reshape(8, 4, 2, mesh.shape["rep"]), (Z, X, C, Y))
    return jax.shard_map(
        local,
        mesh=finer,
        in_specs=(
            P(DEV_REP, None),
            P(DEV_REP, None),
            P(DEV, None),
            P(DEV, None),
            P(DEV_REP, None, None, None),
            P(DEV_REP, None),
            P(DEV_REP, None, None),
            P(DEV_REP, None),
            P(),
            P(),
            P(DEV_REP, None),
        ),
        out_specs=(P(DEV_REP, None), P(DEV, None), P()),
        check_vma=False,
    )
```

```python
import functools
import math

import jax
import jax.numpy as jnp
from jax import lax
from jax.experimental import pallas as pl
from jax.experimental.pallas import tpu as pltpu
from jax.sharding import Mesh
from jax.sharding import PartitionSpec as P

Z, X, C, Y = "dev_0", "dev_1", "dev_2", "rep"
DEV = (Z, X, C)
DEV_REP = (Z, X, C, Y)
AXES = {"z": Z, "x": X, "c": C, "y": Y}
MIB = 1024 * 1024

restart = 0.1
strength = 0.5
BF = jnp.bfloat16
F32 = jnp.float32
VMEM = pltpu.VMEM
SMEM = pltpu.SMEM


def vspec():
    return pl.BlockSpec(memory_space=VMEM)


def sspec():
    return pl.BlockSpec(memory_space=SMEM)


def aspec():
    return pl.BlockSpec(memory_space=pl.ANY)


def cost(flops, nbytes):
    return pl.CostEstimate(flops=int(flops), bytes_accessed=int(nbytes), transcendentals=0)


def pack_kernel(inv_ref, cnt_ref, tiles_ref, extra_ref, out_ref, sem):
    groups = out_ref.shape[0]
    for g in range(groups):
        for d in range(4):
            t = inv_ref[g * 4 + d]
            pltpu.make_async_copy(
                tiles_ref.at[t], out_ref.at[g, pl.ds(0, 128), pl.ds(d * 128, 128)], sem.at[g]
            ).start()
    lane = lax.broadcasted_iota(jnp.int32, (128, 128), 1)

    def one(g, carry):
        for d in range(4):
            pltpu.make_async_copy(
                tiles_ref.at[0], out_ref.at[g, pl.ds(0, 128), pl.ds(d * 128, 128)], sem.at[g]
            ).wait()
        for d in range(4):
            here = (pl.ds(0, 128), pl.ds(d * 128, 128))
            tile = out_ref[g, here[0], here[1]].astype(F32)
            tile = jnp.where(lane < cnt_ref[g * 4 + d], tile, 0.0)
            out_ref[g, here[0], here[1]] = tile.astype(BF)
        out_ref[g, 128:144, :] = extra_ref[g]
        return carry

    lax.fori_loop(0, groups, one, 0)


def packed_tiles(inv, cnt, tiles, extra):
    return pl.pallas_call(
        pack_kernel,
        out_shape=jax.ShapeDtypeStruct((16, 144, 512), BF),
        in_specs=[sspec(), sspec(), aspec(), vspec()],
        out_specs=vspec(),
        scratch_shapes=[pltpu.SemaphoreType.DMA((16,))],
        compiler_params=pltpu.CompilerParams(vmem_limit_bytes=16 * MIB),
        cost_estimate=cost(3e9, 5e6),
    )(inv, cnt, tiles, extra)


def rem(a, n):
    return lax.rem(a + n, n)


def step_kernel(
    idx_ref, pack_ref, hist_a_ref, hist_b_ref, tiles_ref, cols_ref, from_ref, prev_ref, zero_ref,
    weight_two_ref, weight_three_ref, grad_ref,
    three_ref, fresh_ref, term_ref,
    far, own_a, own_b, table, got, rows, vin, idx_in, idx, tiles, home, same, other, partner, sums,
    arrived_a, arrived_b, second, low, share, share_z, share_xc, share_y, whole, far_send, far_recv, y_send, y_recv, idx_send, idx_recv, v_send, v_recv,
    pair_send, pair_recv, sum_send, sum_recv, new_send, new_recv, local_sem,
    gz_send, gz_recv, gxc_send, gxc_recv, gy_send, gy_recv, hxc_send, hxc_recv, hz_send, hz_recv,
):
    z, x, core, turn = (lax.axis_index(a) for a in (Z, X, C, Y))
    hist = (hist_a_ref, hist_b_ref)
    own = (own_a, own_b)
    arrived = (arrived_a, arrived_b)

    def remote(src, dst, send, recv, **to):
        return pltpu.make_async_remote_copy(
            src_ref=src, dst_ref=dst, send_sem=send, recv_sem=recv,
            device_id={AXES[a]: v for a, v in to.items()},
            device_id_type=pl.DeviceIdType.MESH,
        )

    barrier = pltpu.get_barrier_semaphore()

    def greet(**to):
        pl.semaphore_signal(
            barrier, inc=1, device_id={AXES[a]: v for a, v in to.items()},
            device_id_type=pl.DeviceIdType.MESH,
        )

    for by in (1, 2, 3):
        greet(x=rem(x + by, 4))
        greet(x=rem(x + by, 4), c=1 - core)
        greet(y=rem(turn + by, 4))

    def greet_zc(o, carry):
        greet(z=rem(z + o // 2, 8), c=rem(core + o % 2, 2))
        return carry

    lax.fori_loop(1, 16, greet_zc, 0)

    local_copies = [
        pltpu.make_async_copy(hist[0], own_a, local_sem.at[0]),
        pltpu.make_async_copy(hist[1], own_b, local_sem.at[1]),
        pltpu.make_async_copy(tiles_ref.at[:, pl.ds(0, 4)], tiles, local_sem.at[2]),
        pltpu.make_async_copy(idx_ref.at[2 * z + core], idx_in.at[2 * z + core], local_sem.at[3]),
        pltpu.make_async_copy(pack_ref.at[2 * z + core], vin.at[2 * z + core], local_sem.at[4]),
    ]
    for copy in local_copies:
        copy.start()

    def quarter(l, q):
        return hist[l].at[pl.ds(rem(turn + q, 4) * 8, 8)]

    down, up = rem(x + 3, 4), rem(x + 1, 4)

    def along_x(l, n):
        d, q, src, to = (
            (0, 0, None, down), (0, 1, None, down), (2, 1, None, up), (2, 0, None, up),
            (1, 0, far.at[l, 0, 0], down), (1, 1, far.at[l, 2, 1], up),
        )[n]
        src = quarter(l, q) if src is None else src
        return remote(src, far.at[l, d, q], far_send.at[l, n], far_recv.at[l, d, q], x=to)

    def along_y(l, d, q):
        to, at = (rem(turn + 1, 4), 3) if q == 0 else (rem(turn + 3, 4), 2)
        return remote(
            far.at[l, d, q], far.at[l, d, at], y_send.at[l, d, q], y_recv.at[l, d, q], y=to
        )

    def x_here(l, d, q):
        remote(
            far.at[l, d, q], far.at[l, d, q], far_send.at[l, 0], far_recv.at[l, d, q], x=down
        ).wait_recv()

    def y_here(l, d):
        for q in range(2):
            along_y(l, d, q).wait_recv()

    def send_index(o):
        to_z, to_c = rem(z + o // 2, 8), rem(core + o % 2, 2)
        return remote(
            idx_ref.at[2 * to_z + to_c], idx_in.at[2 * z + core],
            idx_send.at[o], idx_recv.at[o], z=to_z, c=to_c,
        )

    def send_pack(o):
        to_z, to_c = rem(z + o // 2, 8), rem(core + o % 2, 2)
        return remote(
            pack_ref.at[2 * to_z + to_c], vin.at[2 * z + core],
            v_send.at[o], v_recv.at[o], z=to_z, c=to_c,
        )

    def each(first, last, act):
        def body(o, carry):
            act(o)
            return carry

        lax.fori_loop(first, last, body, 0)

    pl.semaphore_wait(barrier, 24)
    for n in (0, 2, 1, 3):
        along_x(0, n).start()
    each(1, 16, lambda o: send_index(o).start())
    each(1, 16, lambda o: send_pack(o).start())

    def gather(l, d):
        def widen(s, carry):
            r = pl.multiple_of(s * 128, 128)
            if d == 0:
                block = own[l][rem(s + 8 * turn, 32)]
            else:
                block = far[l, d - 1, s // 8, lax.rem(s, 8)]
            block = block.astype(F32)
            table[pl.ds(2 * r, 128, stride=2), :] = block[:, :128]
            table[pl.ds(2 * r + 1, 128, stride=2), :] = block[:, 128:]
            return carry

        lax.fori_loop(0, 32, widen, 0)

        def worker(g):
            for j in range(128):
                got[pl.ds(2 * j, 2), :] = table[pl.ds(2 * idx[g, d, j], 2), :]
            left, right = got[pl.ds(0, 128, stride=2), :], got[pl.ds(1, 128, stride=2), :]
            both = jnp.concatenate([left, right], axis=1).astype(BF)
            rows[l, g, pl.ds(d * 128, 128), :] = both

        each(0, 16, worker)

    def product(l, n, which):
        g = rem(z + n + 1, 8) * 2 + which
        packed = vin[g, 0:128, :]
        flag = vin[g, 128:129, :]
        both = jnp.concatenate([packed * flag, packed * (1 - flag)], axis=0)
        return jnp.dot(both, rows[l, g], preferred_element_type=F32)

    def to_partner(l, h):
        part = pl.ds(4 * h, 4)
        return remote(
            other.at[l, part], partner.at[l, part], pair_send.at[l, h], pair_recv.at[l, h],
            c=1 - core,
        )

    def send_sum(l, n):
        return remote(
            sums.at[l, pl.ds(2 * n, 2)], arrived[l].at[pl.ds(2 * n, 2)], sum_send.at[l, n], sum_recv.at[l, n],
            z=rem(z + n + 1, 8),
        )

    def plane_sums(l):
        for h in range(2):
            def for_partner(n):
                other[l, n] = product(l, n, 1 - core).astype(BF)

            each(4 * h, 4 * h + 4, for_partner)
            if h:
                to_partner(l, 0).start()

        def for_me(n):
            same[n] = product(l, n, core)

        each(0, 4, for_me)
        to_partner(l, 1).start()
        each(4, 8, for_me)

        def add(n):
            both = (same[n] + partner[l, n].astype(F32)).astype(BF)
            sums[l, pl.ds(2 * n, 2)] = both.reshape(2, 128, 256)

        to_partner(l, 0).wait_recv()
        add(0)

        def add_and_send(n):
            add(n)
            send_sum(l, n - 1).start()

        each(1, 4, add_and_send)
        to_partner(l, 1).wait_recv()
        each(4, 8, add_and_send)

    def at_home(l):
        def block_sum(i):
            total = None
            for t in range(l, 4):
                b = cols_ref[i, t]
                block = own[l][b] if t else prev_ref[b]
                part = jnp.dot(tiles[i, t], block, preferred_element_type=F32)
                total = part if total is None else total + part
            home[l, i] = total

        each(0, 8, block_sum)

    def finish(l, i):
        mine = pl.ds(pl.multiple_of(i * 128, 128), 128)
        total = home[l, i] + arrived[l][from_ref[i, 0]].astype(F32)
        total += arrived[l][from_ref[i, 1]].astype(F32)
        mixed = (1.0 - restart) * total + restart * zero_ref[mine, :].astype(F32)
        factor = math.log(strength / (l + 2) + 1.0)
        rounded = mixed.astype(BF)
        weight = (weight_two_ref, weight_three_ref)[l][...]
        out = jnp.dot(rounded, weight, preferred_element_type=F32)
        out = jnp.maximum((1.0 - factor) * mixed + factor * out, 0.0).astype(BF)
        return mine, rounded, out

    def relay(l):
        x_here(l, 0, 0)
        along_x(l, 4).start()
        along_y(l, 0, 0).start()
        x_here(l, 2, 1)
        along_x(l, 5).start()
        along_y(l, 2, 1).start()

    def second_pair(l):
        x_here(l, 2, 0)
        along_y(l, 2, 0).start()
        x_here(l, 0, 1)
        along_y(l, 0, 1).start()

    def third_pair(l):
        for q in range(2):
            x_here(l, 1, q)
            along_y(l, 1, q).start()

    def arrived_here(l):
        each(0, 7, lambda n: send_sum(l, n).wait_recv())

    for copy in local_copies:
        copy.wait()
    each(1, 16, lambda o: send_index(o).wait_recv())
    to_smem = pltpu.make_async_copy(idx_in, idx, local_sem.at[5])
    to_smem.start()
    to_smem.wait()
    gather(0, 0)
    relay(0)
    for n in (0, 2, 1, 3):
        along_x(1, n).start()
    at_home(0)
    second_pair(0)
    gather(1, 0)
    third_pair(0)
    y_here(0, 0)
    gather(0, 1)
    y_here(0, 2)
    gather(0, 3)
    relay(1)
    y_here(0, 1)
    gather(0, 2)
    each(1, 16, lambda o: send_pack(o).wait_recv())
    plane_sums(0)
    second_pair(1)
    at_home(1)
    third_pair(1)
    y_here(1, 0)
    gather(1, 1)
    y_here(1, 2)
    gather(1, 3)
    arrived_a[14:16] = sums[0, 14:16]
    arrived_here(0)

    def layer_two(i):
        second[i] = finish(0, i)[2]

    each(0, 8, layer_two)
    y_here(1, 1)
    gather(1, 2)
    plane = fresh_ref.at[pl.ds(turn * 8, 8)]
    new_copies = [
        remote(second, plane, new_send.at[s - 1], new_recv.at[s - 1], y=rem(turn + s, 4))
        for s in (1, 2, 3)
    ]
    plane_sums(1)
    for copy in new_copies:
        copy.start()
    keep = pltpu.make_async_copy(second, plane, local_sem.at[6])
    keep.start()

    def add_current(i):
        block = second[cols_ref[i, 0]]
        home[1, i] += jnp.dot(tiles[i, 0], block, preferred_element_type=F32)

    each(0, 8, add_current)
    arrived_b[14:16] = sums[1, 14:16]
    arrived_here(1)

    def layer_three(i):
        mine, rounded, out = finish(1, i)
        three_ref[mine, :] = out
        low[mine, :] = rounded

    each(0, 8, layer_three)
    term = math.log(strength / 3 + 1.0) * lax.dot_general(
        low[...], grad_ref[...], (((0,), (0,)), ((), ())), preferred_element_type=F32
    )
    share[0:32] = term[:, :128].reshape(32, 8, 128)
    share[32:64] = term[:, 128:].reshape(32, 8, 128)
    for copy in new_copies:
        copy.wait_recv()
    keep.wait()

    def xc(o):
        return rem(x + o // 2, 4), rem(core + o % 2, 2)

    def term_z(dz):
        to = rem(z + dz, 8)
        return remote(
            share.at[pl.ds(8 * to, 8)], share_z.at[dz], gz_send.at[dz], gz_recv.at[dz], z=to
        )

    def term_xc(o):
        to_x, to_c = xc(o)
        return remote(
            share_z.at[0, 2 * to_x + to_c], share_xc.at[o], gxc_send.at[o], gxc_recv.at[o],
            x=to_x, c=to_c,
        )

    def term_y(dy):
        return remote(
            share_xc.at[0], share_y.at[turn], gy_send.at[dy], gy_recv.at[dy],
            y=rem(turn + dy, 4),
        )

    mine = 8 * z + 2 * x + core

    def back_xc(o):
        to_x, to_c = xc(o)
        return remote(
            whole.at[mine], whole.at[mine], hxc_send.at[o], hxc_recv.at[o], x=to_x, c=to_c
        )

    def back_z(dz):
        plane = whole.at[pl.ds(8 * z, 8)]
        return remote(plane, plane, hz_send.at[dz], hz_recv.at[dz], z=rem(z + dz, 8))

    each(1, 8, lambda o: term_z(o).start())
    each(1, 8, lambda o: term_z(o).wait_recv())
    total = share[pl.ds(8 * z, 8)]
    for o in range(1, 8):
        total += share_z[o]
    share_z[0] = total
    each(1, 8, lambda o: term_xc(o).start())
    each(1, 8, lambda o: term_xc(o).wait_recv())
    total = share_z[0, 2 * x + core]
    for o in range(1, 8):
        total += share_xc[o]
    share_xc[0] = total
    share_y[turn] = total
    each(1, 4, lambda o: term_y(o).start())
    each(1, 4, lambda o: term_y(o).wait_recv())
    whole[mine] = share_y[0] + share_y[1] + share_y[2] + share_y[3]
    each(1, 8, lambda o: back_xc(o).start())
    each(1, 8, lambda o: back_xc(o).wait_recv())
    each(1, 8, lambda o: back_z(o).start())
    each(1, 8, lambda o: back_z(o).wait_recv())
    term_ref[:, :128] = whole[0:32].reshape(256, 128)
    term_ref[:, 128:] = whole[32:64].reshape(256, 128)
    for copy in (term_z, term_xc, back_xc, back_z):
        each(1, 8, lambda o: copy(o).wait_send())
    each(1, 4, lambda o: term_y(o).wait_send())
    for l in range(2):
        for n in range(6):
            along_x(l, n).wait_send()
        for d in range(3):
            for q in range(2):
                along_y(l, d, q).wait_send()
        for h in range(2):
            to_partner(l, h).wait_send()
        each(0, 7, lambda n: send_sum(l, n).wait_send())
    each(1, 16, lambda o: send_index(o).wait_send())
    each(1, 16, lambda o: send_pack(o).wait_send())
    for copy in new_copies:
        copy.wait_send()


def whole_step(*args):
    dma = pltpu.SemaphoreType.DMA
    return pl.pallas_call(
        step_kernel,
        out_shape=(
            jax.ShapeDtypeStruct((1024, 256), BF),
            jax.ShapeDtypeStruct((32, 128, 256), BF),
            jax.ShapeDtypeStruct((256, 256), F32),
        ),
        in_specs=[aspec(), aspec(), aspec(), aspec(), aspec(), sspec(), sspec()] + [vspec()] * 5,
        out_specs=(vspec(), aspec(), vspec()),
        scratch_shapes=[
            VMEM((2, 3, 4, 8, 128, 256), BF),
            VMEM((32, 128, 256), BF),
            VMEM((32, 128, 256), BF),
            VMEM((8192, 128), F32),
            VMEM((256, 128), F32),
            VMEM((2, 16, 512, 256), BF),
            VMEM((16, 144, 512), BF),
            VMEM((16, 4, 128), jnp.int32),
            SMEM((16, 4, 128), jnp.int32),
            VMEM((8, 4, 128, 128), BF),
            VMEM((2, 8, 128, 256), F32),
            VMEM((8, 256, 256), F32),
            VMEM((2, 8, 256, 256), BF),
            VMEM((2, 8, 256, 256), BF),
            VMEM((2, 16, 128, 256), BF),
            VMEM((16, 128, 256), BF),
            VMEM((16, 128, 256), BF),
            VMEM((8, 128, 256), BF),
            VMEM((1024, 256), BF),
            VMEM((64, 8, 128), F32),
            VMEM((8, 8, 8, 128), F32),
            VMEM((8, 8, 128), F32),
            VMEM((4, 8, 128), F32),
            VMEM((64, 8, 128), F32),
            dma((2, 6)), dma((2, 3, 2)), dma((2, 3, 2)), dma((2, 3, 2)),
            dma((16,)), dma((16,)), dma((16,)), dma((16,)),
            dma((2, 2)), dma((2, 2)), dma((2, 7)), dma((2, 7)), dma((3,)), dma((3,)), dma((7,)),
            dma((8,)), dma((8,)), dma((8,)), dma((8,)), dma((4,)), dma((4,)),
            dma((8,)), dma((8,)), dma((8,)), dma((8,)),
        ],
        compiler_params=pltpu.CompilerParams(
            vmem_limit_bytes=60 * MIB, collective_id=1, has_side_effects=True
        ),
        cost_estimate=cost(60e9, 40e6),
    )(*args)


def local(
    h_zero, h_prev, hist_a, hist_b, tile_vals, tile_cols, pull_rows, pull_counts,
    weight_two, weight_three, grad_out,
):
    x, turn = lax.axis_index(X), lax.axis_index(Y)

    k = lax.broadcasted_iota(jnp.int32, (8, 2, 4), 0)
    c = lax.broadcasted_iota(jnp.int32, (8, 2, 4), 1)
    d = lax.broadcasted_iota(jnp.int32, (8, 2, 4), 2)
    owner = (8 * k + 2 * lax.rem(x + d, 4) + c).reshape(64)
    named = tile_cols[:, 4:].reshape(64) - 40
    block = lax.broadcasted_iota(jnp.int32, (8, 8), 0).reshape(64)
    place = (lax.broadcasted_iota(jnp.int32, (8, 8), 1) + 12 * block.reshape(8, 8) + 4).reshape(64)
    is_it = named[None, :] == jnp.arange(64, dtype=jnp.int32)[:, None]
    tile_of = jnp.sum(jnp.where(is_it, place[None, :], 0), axis=1)
    block_of = jnp.sum(jnp.where(is_it, block[None, :], 0), axis=1).reshape(8, 8)
    ends = jnp.stack([block_of[:, 0], block_of[:, 7]], axis=1)
    first = (block_of == ends[:, :1]).reshape(64)
    inv = jnp.take(tile_of, owner)
    cnt = jnp.take(pull_counts[0], owner)
    rows = lax.rem(jnp.take(pull_rows[0], owner, axis=0) + (4096 - 1024 * turn), 4096)
    flag = jnp.broadcast_to(jnp.take(first, owner)[:, None], (64, 128)).reshape(16, 1, 512)
    extra = jnp.pad(flag.astype(BF), ((0, 0), (0, 15), (0, 0)))
    tiles = packed_tiles(inv, cnt, tile_vals.reshape(96, 128, 128), extra)
    blocks = jnp.arange(8, dtype=jnp.int32)
    plane = jnp.sum(
        jnp.where(ends[:, :, None] == blocks[None, None, :], blocks[:, None, None], 0), axis=0
    ).T
    slots = 2 * lax.rem(lax.axis_index(Z) - plane - 1 + 16, 8) + jnp.arange(2, dtype=jnp.int32)
    near = tile_cols[:, :4] - jnp.array([0, 8, 8, 8], dtype=jnp.int32)
    layer_three, fresh_rows, grad_total = whole_step(
        rows.reshape(16, 4, 128), tiles, hist_a.reshape(32, 128, 256),
        hist_b.reshape(32, 128, 256), tile_vals, near, slots,
        h_prev.reshape(8, 128, 256), h_zero, weight_two, weight_three, grad_out,
    )
    return (layer_three, fresh_rows.reshape(4096, 256), grad_total)


def solution(mesh):
    finer = Mesh(mesh.devices.reshape(8, 4, 2, mesh.shape["rep"]), (Z, X, C, Y))
    return jax.shard_map(
        local,
        mesh=finer,
        in_specs=(
            P(DEV_REP, None),
            P(DEV_REP, None),
            P(DEV, None),
            P(DEV, None),
            P(DEV_REP, None, None, None),
            P(DEV_REP, None),
            P(DEV_REP, None, None),
            P(DEV_REP, None),
            P(),
            P(),
            P(DEV_REP, None),
        ),
        out_specs=(P(DEV_REP, None), P(DEV, None), P()),
        check_vma=False,
    )
```

```python
import functools
import math

import jax
import jax.numpy as jnp
from jax import lax
from jax.experimental import pallas as pl
from jax.experimental.pallas import tpu as pltpu
from jax.sharding import Mesh
from jax.sharding import PartitionSpec as P

Z, X, C, Y = "dev_0", "dev_1", "dev_2", "rep"
DEV = (Z, X, C)
DEV_REP = (Z, X, C, Y)
AXES = {"z": Z, "x": X, "c": C, "y": Y}
MIB = 1024 * 1024
PIECES = 4

restart = 0.1
strength = 0.5
BF = jnp.bfloat16
F32 = jnp.float32
VMEM = pltpu.VMEM
SMEM = pltpu.SMEM


def vspec():
    return pl.BlockSpec(memory_space=VMEM)


def sspec():
    return pl.BlockSpec(memory_space=SMEM)


def aspec():
    return pl.BlockSpec(memory_space=pl.ANY)


def cost(flops, nbytes):
    return pl.CostEstimate(flops=int(flops), bytes_accessed=int(nbytes), transcendentals=0)


def table_kernel(cols_ref, tile_ref, first_ref, near_ref, slots_ref, owner_block):
    z = lax.axis_index(Z)

    def name(i, carry):
        near_ref[i, 0] = cols_ref[i, 0]
        for t in range(1, 4):
            near_ref[i, t] = cols_ref[i, t] - 8
        for t in range(4, 12):
            p = cols_ref[i, t] - 40
            tile_ref[p] = 12 * i + t
            owner_block[p] = i
        return carry

    lax.fori_loop(0, 8, name, 0)

    def plane(k, carry):
        on = lax.rem(z - k + 8, 8)
        place = jnp.where(on == 0, 7, jnp.where(on == 4, 0, on - on // 5))
        i = owner_block[8 * k]
        slots_ref[i, 0] = 2 * place
        slots_ref[owner_block[8 * k + 7], 1] = 2 * place + 1
        for n in range(8):
            first_ref[8 * k + n] = jnp.where(owner_block[8 * k + n] == i, 1, 0)
        return carry

    lax.fori_loop(0, 8, plane, 0)


def tables(cols):
    return pl.pallas_call(
        table_kernel,
        out_shape=[
            jax.ShapeDtypeStruct(shape, jnp.int32) for shape in ((64,), (64,), (8, 4), (8, 2))
        ],
        in_specs=[sspec()],
        out_specs=[sspec()] * 4,
        scratch_shapes=[SMEM((64,), jnp.int32)],
    )(cols)


def publish_kernel(n, *refs):
    ins, outs, held, sems = refs[:n], refs[n : 2 * n], refs[2 * n : 3 * n], refs[3 * n]
    into = [pltpu.make_async_copy(i, h, sems.at[0, k]) for k, (i, h) in enumerate(zip(ins, held))]
    onto = [pltpu.make_async_copy(h, o, sems.at[1, k]) for k, (h, o) in enumerate(zip(held, outs))]
    for copy in into:
        copy.start()
    for first, then in zip(into, onto):
        first.wait()
        then.start()
    for copy in onto:
        copy.wait()


def published(*arrays):
    shapes = [jax.ShapeDtypeStruct(a.shape, a.dtype) for a in arrays]
    n = len(arrays)
    return pl.pallas_call(
        functools.partial(publish_kernel, n),
        out_shape=shapes,
        in_specs=[aspec()] * n,
        out_specs=[aspec()] * n,
        scratch_shapes=[VMEM(a.shape, a.dtype) for a in arrays] + [pltpu.SemaphoreType.DMA((2, n))],
        compiler_params=pltpu.CompilerParams(vmem_limit_bytes=63 * MIB),
        cost_estimate=cost(1e6, 6e6),
    )(*arrays)


def rem(a, n):
    return lax.rem(a + n, n)


def step_kernel(
    tile_ref, first_ref, cols_ref, from_ref, cnt_ref, pull_ref, weight_two_ref, weight_three_ref,
    hist_a_ref, hist_b_ref, tiles_hbm, prev_hbm, zero_hbm, grad_hbm,
    three_ref, fresh_ref, term_ref,
    far, own_a, own_b, prev_ref, zero_ref, grad_ref, table, got, rows, pack_ref, vin, idx_ref, idx_in,
    idx, tiles, home, same, other, partner, sums,
    arrived_a, arrived_b, second, low, three, share, share_c, share_xy, share_z, whole, v_mid, s_mid,
    far_send, far_recv, y_send, y_recv, idx_send, idx_recv, v_send, v_recv,
    pair_send, pair_recv, sum_send, sum_recv, new_send, new_recv, local_sem,
    far_z_send, far_z_recv, gc_sem, gxy_send, gxy_recv, gz_send, gz_recv, hxy_send, hxy_recv,
):
    z, x, core, turn = (lax.axis_index(a) for a in (Z, X, C, Y))
    hist = (hist_a_ref, hist_b_ref)
    own = (own_a, own_b)
    arrived = (arrived_a, arrived_b)

    def remote(src, dst, send, recv, **to):
        return pltpu.make_async_remote_copy(
            src_ref=src, dst_ref=dst, send_sem=send, recv_sem=recv,
            device_id={AXES[a]: v for a, v in to.items()},
            device_id_type=pl.DeviceIdType.MESH,
        )

    barrier = pltpu.get_barrier_semaphore()

    def greet(**to):
        pl.semaphore_signal(
            barrier, inc=1, device_id={AXES[a]: v for a, v in to.items()},
            device_id_type=pl.DeviceIdType.MESH,
        )

    def greet_zc(o, carry):
        greet(z=rem(z + o // 2, 8), c=rem(core + o % 2, 2))
        greet(x=rem(x + o // 4, 4), y=rem(turn + o % 4, 4))
        return carry

    lax.fori_loop(1, 16, greet_zc, 0)

    local_copies = [
        pltpu.make_async_copy(hist[0], own_a, local_sem.at[0]),
        pltpu.make_async_copy(hist[1], own_b, local_sem.at[1]),
        pltpu.make_async_copy(prev_hbm, prev_ref, local_sem.at[3]),
        pltpu.make_async_copy(zero_hbm, zero_ref, local_sem.at[4]),
        pltpu.make_async_copy(grad_hbm, grad_ref, local_sem.at[7]),
    ]
    tiles_copy = pltpu.make_async_copy(tiles_hbm, tiles, local_sem.at[2])
    tiles_copy.start()
    for copy in local_copies:
        copy.start()

    def owner(g, d):
        return 8 * (g // 2) + 2 * lax.rem(x + d, 4) + lax.rem(g, 2)

    def want(g, carry):
        for d in range(4):
            p = owner(g, d)
            row = pull_ref[pl.ds(p, 1), :] + (4096 - 1024 * turn)
            idx_ref[g, d : d + 1, :] = lax.rem(row, 4096)
            idx_ref[g, 4 + d : 5 + d, :] = jnp.full((1, 128), first_ref[p], jnp.int32)
        return carry

    lax.fori_loop(0, 16, want, 0)

    lane = lax.broadcasted_iota(jnp.int32, (128, 128), 1)

    def pack(g, carry):
        for d in range(4):
            p = owner(g, d)
            tile = tiles[tile_ref[p]].astype(F32)
            tile = jnp.where(lane < cnt_ref[0, p], tile, 0.0).astype(BF)
            pack_ref[g, :, d * 128 : (d + 1) * 128] = tile
        return carry

    size = 8 // PIECES
    down, up = rem(x + 3, 4), rem(x + 1, 4)

    def piece(l, d, q, h):
        return far.at[l, d, q, pl.ds(h * size, size)]

    def along_x(l, n, h):
        d, q, relayed, to = (
            (0, 0, None, down), (0, 1, None, down), (2, 1, None, up), (2, 0, None, up),
            (1, 0, (0, 0), down), (1, 1, (2, 1), up),
        )[n]
        if relayed is None:
            src = hist[l].at[pl.ds(rem(turn + q, 4) * 8 + h * size, size)]
        else:
            src = piece(l, *relayed, h)
        return remote(
            src, piece(l, d, q, h), far_send.at[l, n, h], far_recv.at[l, 2 * d + q, h], x=to
        )

    def along_y(l, d, q, h):
        to, at = (rem(turn + 1, 4), 3) if q == 0 else (rem(turn + 3, 4), 2)
        return remote(
            piece(l, d, q, h), piece(l, d, at, h),
            y_send.at[l, 2 * d + q, h], y_recv.at[l, 2 * d + q, h], y=to,
        )

    def x_here(l, d, q, h):
        remote(
            piece(l, d, q, h), piece(l, d, q, h),
            far_send.at[l, 0, h], far_recv.at[l, 2 * d + q, h], x=down,
        ).wait_recv()

    def y_here(l, d):
        for q in range(2):
            for h in range(PIECES):
                along_y(l, d, q, h).wait_recv()

    def own_rows(l):
        for n in (0, 2, 1, 3):
            for h in range(PIECES):
                along_x(l, n, h).start()

    def send_index(o):
        to_z, to_c = rem(z + o // 2, 8), rem(core + o % 2, 2)
        return remote(
            idx_ref.at[2 * to_z + to_c], idx_in.at[2 * z + core],
            idx_send.at[o], idx_recv.at[o], z=to_z, c=to_c,
        )

    def send_pack(o):
        to_z, to_c = rem(z + o // 2, 8), rem(core + o % 2, 2)
        return remote(
            pack_ref.at[2 * to_z + to_c], vin.at[2 * z + core],
            v_send.at[o], v_recv.at[o], z=to_z, c=to_c,
        )

    def pack_out(s):
        to_c = (core, 1 - core)[s]
        return remote(
            pack_ref.at[2 * rem(z + 4, 8) + to_c], v_mid.at[s],
            far_z_send.at[0, s], far_z_recv.at[0, s], z=rem(z + (1, 7)[s], 8),
        )

    def pack_on(s):
        source = rem(z + (7, 1)[s], 8)
        return remote(
            v_mid.at[s], vin.at[2 * source + core],
            v_send.at[8 + s], v_recv.at[8 + s], z=rem(source + 4, 8), c=(core, 1 - core)[s],
        )

    def sum_out(l, s):
        return remote(
            sums.at[l, s], s_mid.at[l, s],
            far_z_send.at[1 + l, s], far_z_recv.at[1 + l, s], z=rem(z + (1, 7)[s], 8),
        )

    def sum_on(l, s):
        return remote(
            s_mid.at[l, s], arrived[l].at[s],
            sum_send.at[l, 7 * s], sum_recv.at[l, 7 * s], z=rem(z + (3, 5)[s], 8),
        )

    def packs(act):
        each(2, 8, act)
        each(10, 16, act)
        act(1)

    def pass_packs():
        for s in range(2):
            pack_out(s).wait_recv()
            pack_on(s).start()

    def pass_sums(l):
        for s in range(2):
            sum_out(l, s).wait_recv()
            sum_on(l, s).start()

    def each(first, last, act):
        def body(o, carry):
            act(o)
            return carry

        lax.fori_loop(first, last, body, 0)

    pl.semaphore_wait(barrier, 30)
    own_rows(0)
    each(1, 16, lambda o: send_index(o).start())
    tiles_copy.wait()
    lax.fori_loop(0, 16, pack, 0)
    idx_in[2 * z + core] = idx_ref[2 * z + core]
    vin[2 * z + core] = pack_ref[2 * z + core]
    for s in range(2):
        pack_out(s).start()
    packs(lambda o: send_pack(o).start())

    def gather(l, d):
        def widen(s, carry):
            r = pl.multiple_of(s * 128, 128)
            if d == 0:
                block = own[l][rem(s + 8 * turn, 32)]
            else:
                block = far[l, d - 1, s // 8, lax.rem(s, 8)]
            block = block.astype(F32)
            table[pl.ds(2 * r, 128, stride=2), :] = block[:, :128]
            table[pl.ds(2 * r + 1, 128, stride=2), :] = block[:, 128:]
            return carry

        lax.fori_loop(0, 32, widen, 0)

        def worker(g):
            for j in range(128):
                got[pl.ds(2 * j, 2), :] = table[pl.ds(2 * idx[g, d, j], 2), :]
            left, right = got[pl.ds(0, 128, stride=2), :], got[pl.ds(1, 128, stride=2), :]
            both = jnp.concatenate([left, right], axis=1).astype(BF)
            rows[l, g, pl.ds(d * 128, 128), :] = both

        each(0, 16, worker)

    def away(n):
        return lax.rem(n + n // 4 + 4 * ((8 - n) // 8), 8)

    def product(l, n, which):
        g = rem(z + away(n), 8) * 2 + which
        packed = vin[g]
        flag = jnp.concatenate([idx_in[g, 4 + d : 5 + d, :] for d in range(4)], axis=1)
        flag = flag.astype(F32).astype(BF)
        both = jnp.concatenate([packed * flag, packed * (1 - flag)], axis=0)
        return jnp.dot(both, rows[l, g], preferred_element_type=F32)

    def to_partner(l, h):
        part = pl.ds(4 * h, 4)
        return remote(
            other.at[l, part], partner.at[l, part], pair_send.at[l, h], pair_recv.at[l, h],
            c=1 - core,
        )

    def send_sum(l, n):
        return remote(
            sums.at[l, pl.ds(2 * n, 2)], arrived[l].at[pl.ds(2 * n, 2)], sum_send.at[l, n], sum_recv.at[l, n],
            z=rem(z + away(n), 8),
        )

    def plane_sums(l):
        for h in range(2):
            def for_partner(n):
                other[l, n] = product(l, n, 1 - core).astype(BF)

            each(4 * h, 4 * h + 4, for_partner)
            if h:
                to_partner(l, 0).start()

        def for_me(n):
            same[n] = product(l, n, core)

        each(0, 4, for_me)
        to_partner(l, 1).start()
        each(4, 8, for_me)

        def add(n):
            both = (same[n] + partner[l, n].astype(F32)).astype(BF)
            sums[l, pl.ds(2 * n, 2)] = both.reshape(2, 128, 256)

        to_partner(l, 0).wait_recv()
        add(0)
        add(1)
        for s in range(2):
            sum_out(l, s).start()

        def add_and_send(n):
            add(n)
            send_sum(l, n - 1).start()

        each(2, 4, add_and_send)
        to_partner(l, 1).wait_recv()
        each(4, 8, add_and_send)

    def at_home(l):
        def block_sum(i):
            total = None
            for t in range(l, 4):
                b = cols_ref[i, t]
                block = own[l][b] if t else prev_ref[b]
                part = jnp.dot(tiles[12 * i + t], block, preferred_element_type=F32)
                total = part if total is None else total + part
            home[l, i] = total

        each(0, 8, block_sum)

    def finish(l, i):
        mine = pl.ds(pl.multiple_of(i * 128, 128), 128)
        total = home[l, i] + arrived[l][from_ref[i, 0]].astype(F32)
        total += arrived[l][from_ref[i, 1]].astype(F32)
        mixed = (1.0 - restart) * total + restart * zero_ref[mine, :].astype(F32)
        factor = math.log(strength / (l + 2) + 1.0)
        rounded = mixed.astype(BF)
        weight = (weight_two_ref, weight_three_ref)[l][...]
        out = jnp.dot(rounded, weight, preferred_element_type=F32)
        out = jnp.maximum((1.0 - factor) * mixed + factor * out, 0.0).astype(BF)
        return mine, rounded, out

    def relay(l):
        for h in range(PIECES):
            for n, d, q in ((4, 0, 0), (5, 2, 1)):
                x_here(l, d, q, h)
                along_x(l, n, h).start()
                along_y(l, d, q, h).start()

    def pass_on(l, *pairs):
        for h in range(PIECES):
            for d, q in pairs:
                x_here(l, d, q, h)
                along_y(l, d, q, h).start()

    def second_pair(l):
        pass_on(l, (2, 0), (0, 1))

    def third_pair(l):
        pass_on(l, (1, 0), (1, 1))

    def arrived_here(l):
        each(1, 7, lambda n: send_sum(l, n).wait_recv())
        for s in range(2):
            sum_on(l, s).wait_recv()

    for copy in local_copies:
        copy.wait()
    each(1, 16, lambda o: send_index(o).wait_recv())
    to_smem = pltpu.make_async_copy(idx_in, idx, local_sem.at[5])
    to_smem.start()
    to_smem.wait()
    relay(0)
    own_rows(1)
    gather(0, 0)
    at_home(0)
    pass_packs()
    second_pair(0)
    gather(1, 0)
    third_pair(0)
    y_here(0, 0)
    gather(0, 1)
    y_here(0, 2)
    gather(0, 3)
    relay(1)
    y_here(0, 1)
    gather(0, 2)
    packs(lambda o: send_pack(o).wait_recv())
    for s in range(2):
        pack_on(s).wait_recv()
    plane_sums(0)
    second_pair(1)
    at_home(1)
    pass_sums(0)
    third_pair(1)
    y_here(1, 0)
    gather(1, 1)
    y_here(1, 2)
    gather(1, 3)
    y_here(1, 1)
    gather(1, 2)
    plane_sums(1)
    arrived_a[14:16] = sums[0, 14:16]
    arrived_here(0)

    def layer_two(i):
        second[i] = finish(0, i)[2]

    each(0, 8, layer_two)
    pass_sums(1)
    plane = fresh_ref.at[pl.ds(turn * 8, 8)]
    new_copies = [
        remote(second, plane, new_send.at[s - 1], new_recv.at[s - 1], y=rem(turn + s, 4))
        for s in (1, 2, 3)
    ]
    for copy in new_copies:
        copy.start()
    keep = pltpu.make_async_copy(second, plane, local_sem.at[6])
    keep.start()

    def add_current(i):
        block = second[cols_ref[i, 0]]
        home[1, i] += jnp.dot(tiles[12 * i], block, preferred_element_type=F32)

    each(0, 8, add_current)
    arrived_b[14:16] = sums[1, 14:16]
    arrived_here(1)

    def layer_three(i):
        mine, rounded, out = finish(1, i)
        three[mine, :] = out
        low[mine, :] = rounded

    each(0, 8, layer_three)
    three_copy = pltpu.make_async_copy(three, three_ref, local_sem.at[1])
    term = math.log(strength / 3 + 1.0) * lax.dot_general(
        low[...], grad_ref[...], (((0,), (0,)), ((), ())), preferred_element_type=F32
    )
    share[0:32] = term[:, :128].reshape(32, 8, 128)
    share[32:64] = term[:, 128:].reshape(32, 8, 128)
    three_copy.start()
    for copy in new_copies:
        copy.wait_recv()
    keep.wait()

    half, theirs = pl.ds(32 * core, 32), pl.ds(32 * (1 - core), 32)
    place = 2 * (4 * x + turn)

    def xy(o):
        return rem(x + o // 4, 4), rem(turn + o % 4, 4)

    def term_c():
        return remote(share.at[theirs], share_c, gc_sem.at[0], gc_sem.at[1], c=1 - core)

    def term_xy(o):
        to_x, to_y = xy(o)
        return remote(
            share_c.at[pl.ds(2 * (4 * to_x + to_y), 2)], share_xy.at[o],
            gxy_send.at[o], gxy_recv.at[o], x=to_x, y=to_y,
        )

    def term_z(dz):
        return remote(
            share_xy.at[0], share_z.at[z], gz_send.at[dz], gz_recv.at[dz], z=rem(z + dz, 8)
        )

    def back_xy(o):
        to_x, to_y = xy(o)
        mine = whole.at[pl.ds(32 * core + place, 2)]
        return remote(mine, mine, hxy_send.at[o], hxy_recv.at[o], x=to_x, y=to_y)

    def back_c():
        return remote(whole.at[half], whole.at[half], gc_sem.at[2], gc_sem.at[3], c=1 - core)

    term_c().start()
    term_c().wait_recv()
    share_c[...] = share_c[...] + share[half]
    each(1, 16, lambda o: term_xy(o).start())
    each(1, 16, lambda o: term_xy(o).wait_recv())
    total = share_c[pl.ds(place, 2)]
    for o in range(1, 16):
        total += share_xy[o]
    share_xy[0] = total
    share_z[z] = total
    each(1, 8, lambda o: term_z(o).start())
    each(1, 8, lambda o: term_z(o).wait_recv())
    total = share_z[0]
    for o in range(1, 8):
        total += share_z[o]
    whole[pl.ds(32 * core + place, 2)] = total
    each(1, 16, lambda o: back_xy(o).start())
    each(1, 16, lambda o: back_xy(o).wait_recv())
    back_c().start()
    back_c().wait_recv()
    term_ref[:, :128] = whole[0:32].reshape(256, 128)
    term_ref[:, 128:] = whole[32:64].reshape(256, 128)
    each(1, 16, lambda o: term_xy(o).wait_send())
    each(1, 8, lambda o: term_z(o).wait_send())
    each(1, 16, lambda o: back_xy(o).wait_send())
    three_copy.wait()
    term_c().wait_send()
    back_c().wait_send()
    for l in range(2):
        for h in range(PIECES):
            for n in range(6):
                along_x(l, n, h).wait_send()
            for d in range(3):
                for q in range(2):
                    along_y(l, d, q, h).wait_send()
        for h in range(2):
            to_partner(l, h).wait_send()
        each(1, 7, lambda n: send_sum(l, n).wait_send())
        for s in range(2):
            sum_out(l, s).wait_send()
            sum_on(l, s).wait_send()
    each(1, 16, lambda o: send_index(o).wait_send())
    packs(lambda o: send_pack(o).wait_send())
    for s in range(2):
        pack_out(s).wait_send()
        pack_on(s).wait_send()
    for copy in new_copies:
        copy.wait_send()


def whole_step(*args):
    dma = pltpu.SemaphoreType.DMA
    return pl.pallas_call(
        step_kernel,
        out_shape=(
            jax.ShapeDtypeStruct((1024, 256), BF),
            jax.ShapeDtypeStruct((32, 128, 256), BF),
            jax.ShapeDtypeStruct((256, 256), F32),
        ),
        in_specs=[sspec()] * 5 + [vspec()] * 3 + [aspec()] * 6,
        out_specs=(aspec(), aspec(), vspec()),
        scratch_shapes=[
            VMEM((2, 3, 4, 8, 128, 256), BF),
            VMEM((32, 128, 256), BF),
            VMEM((32, 128, 256), BF),
            VMEM((8, 128, 256), BF),
            VMEM((1024, 256), BF),
            VMEM((1024, 256), BF),
            VMEM((8192, 128), F32),
            VMEM((256, 128), F32),
            VMEM((2, 16, 512, 256), BF),
            VMEM((16, 128, 512), BF),
            VMEM((16, 128, 512), BF),
            VMEM((16, 8, 128), jnp.int32),
            VMEM((16, 8, 128), jnp.int32),
            SMEM((16, 8, 128), jnp.int32),
            VMEM((96, 128, 128), BF),
            VMEM((2, 8, 128, 256), F32),
            VMEM((8, 256, 256), F32),
            VMEM((2, 8, 256, 256), BF),
            VMEM((2, 8, 256, 256), BF),
            VMEM((2, 16, 128, 256), BF),
            VMEM((16, 128, 256), BF),
            VMEM((16, 128, 256), BF),
            VMEM((8, 128, 256), BF),
            VMEM((1024, 256), BF),
            VMEM((1024, 256), BF),
            VMEM((64, 8, 128), F32),
            VMEM((32, 8, 128), F32),
            VMEM((16, 2, 8, 128), F32),
            VMEM((8, 2, 8, 128), F32),
            VMEM((64, 8, 128), F32),
            VMEM((2, 128, 512), BF),
            VMEM((2, 2, 128, 256), BF),
            dma((2, 6, PIECES)), dma((2, 6, PIECES)), dma((2, 6, PIECES)), dma((2, 6, PIECES)),
            dma((16,)), dma((16,)), dma((16,)), dma((16,)),
            dma((2, 2)), dma((2, 2)), dma((2, 8)), dma((2, 8)), dma((3,)), dma((3,)), dma((8,)),
            dma((3, 2)), dma((3, 2)), dma((4,)), dma((16,)), dma((16,)), dma((8,)), dma((8,)),
            dma((16,)), dma((16,)),
        ],
        compiler_params=pltpu.CompilerParams(
            vmem_limit_bytes=60 * MIB, collective_id=1, has_side_effects=True
        ),
        cost_estimate=cost(60e9, 40e6),
    )(*args)


def local(
    h_zero, h_prev, hist_a, hist_b, tile_vals, tile_cols, pull_rows, pull_counts,
    weight_two, weight_three, grad_out,
):
    tile_of, first, near, slots = tables(tile_cols)
    outs = whole_step(
        tile_of, first, near, slots, pull_counts, pull_rows.reshape(64, 128),
        weight_two, weight_three, hist_a.reshape(32, 128, 256), hist_b.reshape(32, 128, 256),
        tile_vals.reshape(96, 128, 128), h_prev.reshape(8, 128, 256), h_zero, grad_out,
    )
    layer_three, fresh_rows, grad_total = published(*outs)
    return (layer_three, fresh_rows.reshape(4096, 256), grad_total)


def solution(mesh):
    finer = Mesh(mesh.devices.reshape(8, 4, 2, mesh.shape["rep"]), (Z, X, C, Y))
    return jax.shard_map(
        local,
        mesh=finer,
        in_specs=(
            P(DEV_REP, None),
            P(DEV_REP, None),
            P(DEV, None),
            P(DEV, None),
            P(DEV_REP, None, None, None),
            P(DEV_REP, None),
            P(DEV_REP, None, None),
            P(DEV_REP, None),
            P(),
            P(),
            P(DEV_REP, None),
        ),
        out_specs=(P(DEV_REP, None), P(DEV, None), P()),
        check_vma=False,
    )
```

```python
import functools
import math

import jax
import jax.numpy as jnp
from jax import lax
from jax.experimental import pallas as pl
from jax.experimental.pallas import tpu as pltpu
from jax.sharding import Mesh
from jax.sharding import PartitionSpec as P

Z, X, C, Y = "dev_0", "dev_1", "dev_2", "rep"
DEV = (Z, X, C)
DEV_REP = (Z, X, C, Y)
AXES = {"z": Z, "x": X, "c": C, "y": Y}
MIB = 1024 * 1024
PIECES = 4
WIDTHS = (256, 128, 128)

restart = 0.1
strength = 0.5
BF = jnp.bfloat16
F32 = jnp.float32
VMEM = pltpu.VMEM
SMEM = pltpu.SMEM


def vspec():
    return pl.BlockSpec(memory_space=VMEM)


def sspec():
    return pl.BlockSpec(memory_space=SMEM)


def aspec():
    return pl.BlockSpec(memory_space=pl.ANY)


def cost(flops, nbytes):
    return pl.CostEstimate(flops=int(flops), bytes_accessed=int(nbytes), transcendentals=0)


def table_kernel(cols_ref, tile_ref, first_ref, near_ref, slots_ref, owner_block):
    z = lax.axis_index(Z)

    def name(i, carry):
        near_ref[i, 0] = cols_ref[i, 0]
        for t in range(1, 4):
            near_ref[i, t] = cols_ref[i, t] - 8
        for t in range(4, 12):
            p = cols_ref[i, t] - 40
            tile_ref[p] = 12 * i + t
            owner_block[p] = i
        return carry

    lax.fori_loop(0, 8, name, 0)

    def plane(k, carry):
        on = lax.rem(z - k + 8, 8)
        place = jnp.where(on == 0, 7, jnp.where(on == 4, 0, on - on // 5))
        i = owner_block[8 * k]
        slots_ref[i, 0] = 2 * place
        slots_ref[owner_block[8 * k + 7], 1] = 2 * place + 1
        for n in range(8):
            first_ref[8 * k + n] = jnp.where(owner_block[8 * k + n] == i, 1, 0)
        return carry

    lax.fori_loop(0, 8, plane, 0)


def tables(cols):
    return pl.pallas_call(
        table_kernel,
        out_shape=[
            jax.ShapeDtypeStruct(shape, jnp.int32) for shape in ((64,), (64,), (8, 4), (8, 2))
        ],
        in_specs=[sspec()],
        out_specs=[sspec()] * 4,
        scratch_shapes=[SMEM((64,), jnp.int32)],
    )(cols)


def publish_kernel(n, *refs):
    ins, outs, held, sems = refs[:n], refs[n : 2 * n], refs[2 * n : 3 * n], refs[3 * n]
    into = [pltpu.make_async_copy(i, h, sems.at[0, k]) for k, (i, h) in enumerate(zip(ins, held))]
    onto = [pltpu.make_async_copy(h, o, sems.at[1, k]) for k, (h, o) in enumerate(zip(held, outs))]
    for copy in into:
        copy.start()
    for first, then in zip(into, onto):
        first.wait()
        then.start()
    for copy in onto:
        copy.wait()


def published(*arrays):
    shapes = [jax.ShapeDtypeStruct(a.shape, a.dtype) for a in arrays]
    n = len(arrays)
    return pl.pallas_call(
        functools.partial(publish_kernel, n),
        out_shape=shapes,
        in_specs=[aspec()] * n,
        out_specs=[aspec()] * n,
        scratch_shapes=[VMEM(a.shape, a.dtype) for a in arrays] + [pltpu.SemaphoreType.DMA((2, n))],
        compiler_params=pltpu.CompilerParams(vmem_limit_bytes=63 * MIB),
        cost_estimate=cost(1e6, 6e6),
    )(*arrays)


def rem(a, n):
    return lax.rem(a + n, n)


def step_kernel(
    tile_ref, first_ref, cols_ref, from_ref, cnt_ref, pull_ref, weight_two_ref, weight_three_ref,
    hist_a_ref, hist_b_ref, tiles_hbm, prev_hbm, zero_hbm, grad_hbm,
    three_ref, fresh_ref, term_ref,
    *refs,
):
    refs = iter(refs)
    far, rows, same, other, partner, sums, s_mid, arrived = (
        [next(refs) for _ in range(3)] for _ in range(8)
    )
    (
        own_a, own_b, prev_ref, zero_ref, grad_ref, table, got, pack_ref, vin, idx_ref, idx_in,
        idx, tiles, home, second, low, three, share, share_c, share_xy, share_z, whole, v_mid,
        far_send, far_recv, y_send, y_recv, idx_send, idx_recv, v_send, v_recv,
        pair_send, pair_recv, sum_send, sum_recv, new_send, new_recv, local_sem,
        far_z_send, far_z_recv, gc_sem, gxy_send, gxy_recv, gz_send, gz_recv, hxy_send, hxy_recv,
    ) = refs
    z, x, core, turn = (lax.axis_index(a) for a in (Z, X, C, Y))
    hist = (hist_a_ref, hist_b_ref)
    own = (own_a, own_b)
    layer = (0, 1, 1)

    def remote(src, dst, send, recv, **to):
        return pltpu.make_async_remote_copy(
            src_ref=src, dst_ref=dst, send_sem=send, recv_sem=recv,
            device_id={AXES[a]: v for a, v in to.items()},
            device_id_type=pl.DeviceIdType.MESH,
        )

    barrier = pltpu.get_barrier_semaphore()

    def greet(**to):
        pl.semaphore_signal(
            barrier, inc=1, device_id={AXES[a]: v for a, v in to.items()},
            device_id_type=pl.DeviceIdType.MESH,
        )

    def greet_zc(o, carry):
        greet(z=rem(z + o // 2, 8), c=rem(core + o % 2, 2))
        greet(x=rem(x + o // 4, 4), y=rem(turn + o % 4, 4))
        return carry

    lax.fori_loop(1, 16, greet_zc, 0)

    local_copies = [
        pltpu.make_async_copy(hist[0], own_a, local_sem.at[0]),
        pltpu.make_async_copy(hist[1], own_b, local_sem.at[1]),
        pltpu.make_async_copy(prev_hbm, prev_ref, local_sem.at[3]),
        pltpu.make_async_copy(zero_hbm, zero_ref, local_sem.at[4]),
        pltpu.make_async_copy(grad_hbm, grad_ref, local_sem.at[7]),
    ]
    tiles_copy = pltpu.make_async_copy(tiles_hbm, tiles, local_sem.at[2])
    tiles_copy.start()
    for copy in local_copies:
        copy.start()

    def owner(g, d):
        return 8 * (g // 2) + 2 * lax.rem(x + d, 4) + lax.rem(g, 2)

    def want(g, carry):
        for d in range(4):
            p = owner(g, d)
            row = pull_ref[pl.ds(p, 1), :] + (4096 - 1024 * turn)
            idx_ref[g, d : d + 1, :] = lax.rem(row, 4096)
            idx_ref[g, 4 + d : 5 + d, :] = jnp.full((1, 128), first_ref[p], jnp.int32)
        return carry

    lax.fori_loop(0, 16, want, 0)

    lane = lax.broadcasted_iota(jnp.int32, (128, 128), 1)

    def pack(g, carry):
        for d in range(4):
            p = owner(g, d)
            tile = tiles[tile_ref[p]].astype(F32)
            tile = jnp.where(lane < cnt_ref[0, p], tile, 0.0).astype(BF)
            pack_ref[g, :, d * 128 : (d + 1) * 128] = tile
        return carry

    size = 8 // PIECES
    down, up = rem(x + 3, 4), rem(x + 1, 4)

    def piece(l, d, q, h):
        return far[l].at[d, q, pl.ds(h * size, size)]

    def along_x(l, n, h):
        d, q, relayed, to = (
            (0, 0, None, down), (0, 1, None, down), (2, 1, None, up), (2, 0, None, up),
            (1, 0, (0, 0), down), (1, 1, (2, 1), up),
        )[n]
        if relayed is None:
            src = hist[layer[l]].at[pl.ds(rem(turn + q, 4) * 8 + h * size, size)]
            if l:
                src = src.at[:, :, pl.ds(128 * (l - 1), 128)]
        else:
            src = piece(l, *relayed, h)
        return remote(
            src, piece(l, d, q, h), far_send.at[l, n, h], far_recv.at[l, 2 * d + q, h], x=to
        )

    def along_y(l, d, q, h):
        to, at = (rem(turn + 1, 4), 3) if q == 0 else (rem(turn + 3, 4), 2)
        return remote(
            piece(l, d, q, h), piece(l, d, at, h),
            y_send.at[l, 2 * d + q, h], y_recv.at[l, 2 * d + q, h], y=to,
        )

    def x_here(l, d, q, h):
        remote(
            piece(l, d, q, h), piece(l, d, q, h),
            far_send.at[l, 0, h], far_recv.at[l, 2 * d + q, h], x=down,
        ).wait_recv()

    def y_here(l, d):
        for q in range(2):
            for h in range(PIECES):
                along_y(l, d, q, h).wait_recv()

    def own_rows(l):
        for n in (0, 2, 1, 3):
            for h in range(PIECES):
                along_x(l, n, h).start()

    def send_index(o):
        to_z, to_c = rem(z + o // 2, 8), rem(core + o % 2, 2)
        return remote(
            idx_ref.at[2 * to_z + to_c], idx_in.at[2 * z + core],
            idx_send.at[o], idx_recv.at[o], z=to_z, c=to_c,
        )

    def send_pack(o):
        to_z, to_c = rem(z + o // 2, 8), rem(core + o % 2, 2)
        return remote(
            pack_ref.at[2 * to_z + to_c], vin.at[2 * z + core],
            v_send.at[o], v_recv.at[o], z=to_z, c=to_c,
        )

    def pack_out(s):
        to_c = (core, 1 - core)[s]
        return remote(
            pack_ref.at[2 * rem(z + 4, 8) + to_c], v_mid.at[s],
            far_z_send.at[0, s], far_z_recv.at[0, s], z=rem(z + (1, 7)[s], 8),
        )

    def pack_on(s):
        source = rem(z + (7, 1)[s], 8)
        return remote(
            v_mid.at[s], vin.at[2 * source + core],
            v_send.at[8 + s], v_recv.at[8 + s], z=rem(source + 4, 8), c=(core, 1 - core)[s],
        )

    def sum_out(l, s):
        return remote(
            sums[l].at[s], s_mid[l].at[s],
            far_z_send.at[1 + l, s], far_z_recv.at[1 + l, s], z=rem(z + (1, 7)[s], 8),
        )

    def sum_on(l, s):
        return remote(
            s_mid[l].at[s], arrived[l].at[s],
            sum_send.at[l, 7 * s], sum_recv.at[l, 7 * s], z=rem(z + (3, 5)[s], 8),
        )

    def packs(act):
        each(2, 8, act)
        each(10, 16, act)
        act(1)

    def pass_packs():
        for s in range(2):
            pack_out(s).wait_recv()
            pack_on(s).start()

    def pass_sums(l):
        for s in range(2):
            sum_out(l, s).wait_recv()
            sum_on(l, s).start()

    def each(first, last, act):
        def body(o, carry):
            act(o)
            return carry

        lax.fori_loop(first, last, body, 0)

    pl.semaphore_wait(barrier, 30)
    own_rows(0)
    each(1, 16, lambda o: send_index(o).start())
    tiles_copy.wait()
    lax.fori_loop(0, 16, pack, 0)
    idx_in[2 * z + core] = idx_ref[2 * z + core]
    vin[2 * z + core] = pack_ref[2 * z + core]
    for s in range(2):
        pack_out(s).start()
    packs(lambda o: send_pack(o).start())

    def gather(l, d):
        def widen(s, carry):
            r = pl.multiple_of(s * 128, 128)
            if d == 0:
                block = own[layer[l]][rem(s + 8 * turn, 32)]
                if l:
                    block = block[:, 128 * (l - 1) : 128 * l]
            else:
                block = far[l][d - 1, s // 8, lax.rem(s, 8)]
            block = block.astype(F32)
            if l:
                table[pl.ds(r, 128), :] = block
            else:
                table[pl.ds(2 * r, 128, stride=2), :] = block[:, :128]
                table[pl.ds(2 * r + 1, 128, stride=2), :] = block[:, 128:]
            return carry

        lax.fori_loop(0, 32, widen, 0)

        def worker(g):
            if l:
                for j in range(128):
                    got[pl.ds(j, 1), :] = table[pl.ds(idx[g, d, j], 1), :]
                both = got[0:128, :].astype(BF)
            else:
                for j in range(128):
                    got[pl.ds(2 * j, 2), :] = table[pl.ds(2 * idx[g, d, j], 2), :]
                left, right = got[pl.ds(0, 128, stride=2), :], got[pl.ds(1, 128, stride=2), :]
                both = jnp.concatenate([left, right], axis=1).astype(BF)
            rows[l][g, pl.ds(d * 128, 128), :] = both

        each(0, 16, worker)

    def away(n):
        return lax.rem(n + n // 4 + 4 * ((8 - n) // 8), 8)

    def product(l, n, which):
        g = rem(z + away(n), 8) * 2 + which
        packed = vin[g]
        flag = jnp.concatenate([idx_in[g, 4 + d : 5 + d, :] for d in range(4)], axis=1)
        flag = flag.astype(F32).astype(BF)
        both = jnp.concatenate([packed * flag, packed * (1 - flag)], axis=0)
        return jnp.dot(both, rows[l][g], preferred_element_type=F32)

    def to_partner(l, h):
        part = pl.ds(4 * h, 4)
        return remote(
            other[l].at[part], partner[l].at[part], pair_send.at[l, h], pair_recv.at[l, h],
            c=1 - core,
        )

    def send_sum(l, n):
        return remote(
            sums[l].at[pl.ds(2 * n, 2)], arrived[l].at[pl.ds(2 * n, 2)], sum_send.at[l, n], sum_recv.at[l, n],
            z=rem(z + away(n), 8),
        )

    def plane_sums(l):
        for h in range(2):
            def for_partner(n):
                other[l][n] = product(l, n, 1 - core).astype(BF)

            each(4 * h, 4 * h + 4, for_partner)
            if h:
                to_partner(l, 0).start()

        def for_me(n):
            same[l][n] = product(l, n, core)

        each(0, 4, for_me)
        to_partner(l, 1).start()
        each(4, 8, for_me)

        def add(n):
            both = (same[l][n] + partner[l][n].astype(F32)).astype(BF)
            sums[l][pl.ds(2 * n, 2)] = both.reshape(2, 128, both.shape[1])

        to_partner(l, 0).wait_recv()
        add(0)
        add(1)
        for s in range(2):
            sum_out(l, s).start()

        def add_and_send(n):
            add(n)
            send_sum(l, n - 1).start()

        each(2, 4, add_and_send)
        to_partner(l, 1).wait_recv()
        each(4, 8, add_and_send)

    def at_home(l):
        def block_sum(i):
            total = None
            for t in range(l, 4):
                b = cols_ref[i, t]
                block = own[l][b] if t else prev_ref[b]
                part = jnp.dot(tiles[12 * i + t], block, preferred_element_type=F32)
                total = part if total is None else total + part
            home[l, i] = total

        each(0, 8, block_sum)

    def finish(l, i):
        mine = pl.ds(pl.multiple_of(i * 128, 128), 128)
        parts = [
            arrived[st][from_ref[i, 0]].astype(F32) + arrived[st][from_ref[i, 1]].astype(F32)
            for st in range(3) if layer[st] == l
        ]
        total = home[l, i] + (parts[0] if l == 0 else jnp.concatenate(parts, axis=1))
        mixed = (1.0 - restart) * total + restart * zero_ref[mine, :].astype(F32)
        factor = math.log(strength / (l + 2) + 1.0)
        rounded = mixed.astype(BF)
        weight = (weight_two_ref, weight_three_ref)[l][...]
        out = jnp.dot(rounded, weight, preferred_element_type=F32)
        out = jnp.maximum((1.0 - factor) * mixed + factor * out, 0.0).astype(BF)
        return mine, rounded, out

    def relay(l):
        for h in range(PIECES):
            for n, d, q in ((4, 0, 0), (5, 2, 1)):
                x_here(l, d, q, h)
                along_x(l, n, h).start()
                along_y(l, d, q, h).start()

    def pass_on(l, *pairs):
        for h in range(PIECES):
            for d, q in pairs:
                x_here(l, d, q, h)
                along_y(l, d, q, h).start()

    def second_pair(l):
        pass_on(l, (2, 0), (0, 1))

    def third_pair(l):
        pass_on(l, (1, 0), (1, 1))

    def arrived_here(l):
        each(1, 7, lambda n: send_sum(l, n).wait_recv())
        for s in range(2):
            sum_on(l, s).wait_recv()

    for copy in local_copies:
        copy.wait()
    relay(0)
    own_rows(1)
    each(1, 16, lambda o: send_index(o).wait_recv())
    to_smem = pltpu.make_async_copy(idx_in, idx, local_sem.at[5])
    to_smem.start()
    to_smem.wait()
    gather(0, 0)
    at_home(0)
    pass_packs()
    second_pair(0)
    gather(1, 0)
    gather(2, 0)
    third_pair(0)
    y_here(0, 0)
    gather(0, 1)
    y_here(0, 2)
    gather(0, 3)
    relay(1)
    own_rows(2)
    y_here(0, 1)
    gather(0, 2)
    second_pair(1)
    packs(lambda o: send_pack(o).wait_recv())
    for s in range(2):
        pack_on(s).wait_recv()
    plane_sums(0)
    third_pair(1)
    at_home(1)
    pass_sums(0)
    y_here(1, 0)
    gather(1, 1)
    relay(2)
    y_here(1, 2)
    gather(1, 3)
    second_pair(2)
    y_here(1, 1)
    gather(1, 2)
    plane_sums(1)
    third_pair(2)
    y_here(2, 0)
    gather(2, 1)
    y_here(2, 2)
    gather(2, 3)
    pass_sums(1)
    y_here(2, 1)
    gather(2, 2)
    plane_sums(2)
    for st in range(3):
        arrived[st][14:16] = sums[st][14:16]
    arrived_here(0)

    def layer_two(i):
        second[i] = finish(0, i)[2]

    each(0, 8, layer_two)

    def add_current(i):
        block = second[cols_ref[i, 0]]
        home[1, i] += jnp.dot(tiles[12 * i], block, preferred_element_type=F32)

    each(0, 8, add_current)
    keep = pltpu.make_async_copy(second, fresh_ref.at[pl.ds(turn * 8, 8)], local_sem.at[6])
    keep.start()

    def new_rows(way, h, on):
        at = rem(turn + (0 if not on else (3, 1)[way]), 4) * 8 + 4 * h
        there = fresh_ref.at[pl.ds(at, 4)]
        here = there if on else second.at[pl.ds(4 * h, 4)]
        n = 3 * way + (2 if on else h)
        return remote(here, there, new_send.at[n], new_recv.at[n], y=rem(turn + (1, 3)[way], 4))

    def new_here(way, n):
        at = rem(turn + (2 if n == 2 else (3, 1)[way]), 4) * 8 + 4 * (way if n == 2 else n)
        half = fresh_ref.at[pl.ds(at, 4)]
        remote(
            half, half, new_send.at[3 * way], new_recv.at[3 * way + n], y=rem(turn + 1, 4)
        ).wait_recv()

    for h in range(2):
        for way in range(2):
            new_rows(way, (h, 1 - h)[way], False).start()
    pass_sums(2)
    for way in range(2):
        new_here(way, way)
        new_rows(way, way, True).start()
    arrived_here(1)
    arrived_here(2)

    def layer_three(i):
        mine, rounded, out = finish(1, i)
        three[mine, :] = out
        low[mine, :] = rounded

    each(0, 8, layer_three)
    three_copy = pltpu.make_async_copy(three, three_ref, local_sem.at[1])
    term = math.log(strength / 3 + 1.0) * lax.dot_general(
        low[...], grad_ref[...], (((0,), (0,)), ((), ())), preferred_element_type=F32
    )
    share[0:32] = term[:, :128].reshape(32, 8, 128)
    share[32:64] = term[:, 128:].reshape(32, 8, 128)
    three_copy.start()

    half, theirs = pl.ds(32 * core, 32), pl.ds(32 * (1 - core), 32)
    place = 2 * (4 * x + turn)

    def xy(o):
        return rem(x + o // 4, 4), rem(turn + o % 4, 4)

    def term_c():
        return remote(share.at[theirs], share_c, gc_sem.at[0], gc_sem.at[1], c=1 - core)

    def term_xy(o):
        to_x, to_y = xy(o)
        return remote(
            share_c.at[pl.ds(2 * (4 * to_x + to_y), 2)], share_xy.at[o],
            gxy_send.at[o], gxy_recv.at[o], x=to_x, y=to_y,
        )

    def term_z(dz):
        return remote(
            share_xy.at[0], share_z.at[z], gz_send.at[dz], gz_recv.at[dz], z=rem(z + dz, 8)
        )

    def back_xy(o):
        to_x, to_y = xy(o)
        mine = whole.at[pl.ds(32 * core + place, 2)]
        return remote(mine, mine, hxy_send.at[o], hxy_recv.at[o], x=to_x, y=to_y)

    def back_c():
        return remote(whole.at[half], whole.at[half], gc_sem.at[2], gc_sem.at[3], c=1 - core)

    term_c().start()
    term_c().wait_recv()
    share_c[...] = share_c[...] + share[half]
    each(1, 16, lambda o: term_xy(o).start())
    each(1, 16, lambda o: term_xy(o).wait_recv())
    total = share_c[pl.ds(place, 2)]
    for o in range(1, 16):
        total += share_xy[o]
    share_xy[0] = total
    share_z[z] = total
    each(1, 8, lambda o: term_z(o).start())
    each(1, 8, lambda o: term_z(o).wait_recv())
    total = share_z[0]
    for o in range(1, 8):
        total += share_z[o]
    whole[pl.ds(32 * core + place, 2)] = total
    each(1, 16, lambda o: back_xy(o).start())
    each(1, 16, lambda o: back_xy(o).wait_recv())
    back_c().start()
    back_c().wait_recv()
    term_ref[:, :128] = whole[0:32].reshape(256, 128)
    term_ref[:, 128:] = whole[32:64].reshape(256, 128)
    each(1, 16, lambda o: term_xy(o).wait_send())
    each(1, 8, lambda o: term_z(o).wait_send())
    each(1, 16, lambda o: back_xy(o).wait_send())
    three_copy.wait()
    term_c().wait_send()
    back_c().wait_send()
    for l in range(3):
        for h in range(PIECES):
            for n in range(6):
                along_x(l, n, h).wait_send()
            for d in range(3):
                for q in range(2):
                    along_y(l, d, q, h).wait_send()
        for h in range(2):
            to_partner(l, h).wait_send()
        each(1, 7, lambda n: send_sum(l, n).wait_send())
        for s in range(2):
            sum_out(l, s).wait_send()
            sum_on(l, s).wait_send()
    each(1, 16, lambda o: send_index(o).wait_send())
    packs(lambda o: send_pack(o).wait_send())
    for s in range(2):
        pack_out(s).wait_send()
        pack_on(s).wait_send()
    keep.wait()
    for way in range(2):
        for n in (1 - way, 2):
            new_here(way, n)
        for h in range(2):
            new_rows(way, h, False).wait_send()
        new_rows(way, way, True).wait_send()


def whole_step(*args):
    dma = pltpu.SemaphoreType.DMA
    return pl.pallas_call(
        step_kernel,
        out_shape=(
            jax.ShapeDtypeStruct((1024, 256), BF),
            jax.ShapeDtypeStruct((32, 128, 256), BF),
            jax.ShapeDtypeStruct((256, 256), F32),
        ),
        in_specs=[sspec()] * 5 + [vspec()] * 3 + [aspec()] * 6,
        out_specs=(aspec(), aspec(), vspec()),
        scratch_shapes=[
            *(VMEM((3, 4, 8, 128, w), BF) for w in WIDTHS),
            *(VMEM((16, 512, w), BF) for w in WIDTHS),
            *(VMEM((8, 256, w), F32) for w in WIDTHS),
            *(VMEM((8, 256, w), BF) for w in WIDTHS),
            *(VMEM((8, 256, w), BF) for w in WIDTHS),
            *(VMEM((16, 128, w), BF) for w in WIDTHS),
            *(VMEM((2, 128, w), BF) for w in WIDTHS),
            *(VMEM((16, 128, w), BF) for w in WIDTHS),
            VMEM((32, 128, 256), BF),
            VMEM((32, 128, 256), BF),
            VMEM((8, 128, 256), BF),
            VMEM((1024, 256), BF),
            VMEM((1024, 256), BF),
            VMEM((8192, 128), F32),
            VMEM((256, 128), F32),
            VMEM((16, 128, 512), BF),
            VMEM((16, 128, 512), BF),
            VMEM((16, 8, 128), jnp.int32),
            VMEM((16, 8, 128), jnp.int32),
            SMEM((16, 8, 128), jnp.int32),
            VMEM((96, 128, 128), BF),
            VMEM((2, 8, 128, 256), F32),
            VMEM((8, 128, 256), BF),
            VMEM((1024, 256), BF),
            VMEM((1024, 256), BF),
            VMEM((64, 8, 128), F32),
            VMEM((32, 8, 128), F32),
            VMEM((16, 2, 8, 128), F32),
            VMEM((8, 2, 8, 128), F32),
            VMEM((64, 8, 128), F32),
            VMEM((2, 128, 512), BF),
            *(dma((3, 6, PIECES)) for _ in range(4)),
            dma((16,)), dma((16,)), dma((16,)), dma((16,)),
            dma((3, 2)), dma((3, 2)), dma((3, 8)), dma((3, 8)), dma((6,)), dma((6,)), dma((8,)),
            dma((4, 2)), dma((4, 2)), dma((4,)), dma((16,)), dma((16,)), dma((8,)), dma((8,)),
            dma((16,)), dma((16,)),
        ],
        compiler_params=pltpu.CompilerParams(
            vmem_limit_bytes=63 * MIB, collective_id=1, has_side_effects=True
        ),
        cost_estimate=cost(60e9, 40e6),
    )(*args)


def local(
    h_zero, h_prev, hist_a, hist_b, tile_vals, tile_cols, pull_rows, pull_counts,
    weight_two, weight_three, grad_out,
):
    tile_of, first, near, slots = tables(tile_cols)
    outs = whole_step(
        tile_of, first, near, slots, pull_counts, pull_rows.reshape(64, 128),
        weight_two, weight_three, hist_a.reshape(32, 128, 256), hist_b.reshape(32, 128, 256),
        tile_vals.reshape(96, 128, 128), h_prev.reshape(8, 128, 256), h_zero, grad_out,
    )
    layer_three, fresh_rows, grad_total = published(*outs)
    return (layer_three, fresh_rows.reshape(4096, 256), grad_total)


def solution(mesh):
    finer = Mesh(mesh.devices.reshape(8, 4, 2, mesh.shape["rep"]), (Z, X, C, Y))
    return jax.shard_map(
        local,
        mesh=finer,
        in_specs=(
            P(DEV_REP, None),
            P(DEV_REP, None),
            P(DEV, None),
            P(DEV, None),
            P(DEV_REP, None, None, None),
            P(DEV_REP, None),
            P(DEV_REP, None, None),
            P(DEV_REP, None),
            P(),
            P(),
            P(DEV_REP, None),
        ),
        out_specs=(P(DEV_REP, None), P(DEV, None), P()),
        check_vma=False,
    )
```

```python
import functools
import math

import jax
import jax.numpy as jnp
from jax import lax
from jax.experimental import pallas as pl
from jax.experimental.pallas import tpu as pltpu
from jax.sharding import Mesh
from jax.sharding import PartitionSpec as P

Z, X, C, Y = "dev_0", "dev_1", "dev_2", "rep"
DEV = (Z, X, C)
DEV_REP = (Z, X, C, Y)
AXES = {"z": Z, "x": X, "c": C, "y": Y}
MIB = 1024 * 1024
PIECES = 4
WIDTHS = (256, 128, 128)

restart = 0.1
strength = 0.5
BF = jnp.bfloat16
F32 = jnp.float32
VMEM = pltpu.VMEM
SMEM = pltpu.SMEM


def vspec():
    return pl.BlockSpec(memory_space=VMEM)


def sspec():
    return pl.BlockSpec(memory_space=SMEM)


def aspec():
    return pl.BlockSpec(memory_space=pl.ANY)


def cost(flops, nbytes):
    return pl.CostEstimate(flops=int(flops), bytes_accessed=int(nbytes), transcendentals=0)


def table_kernel(cols_ref, tile_ref, first_ref, near_ref, slots_ref, owner_block):
    z = lax.axis_index(Z)

    def name(i, carry):
        near_ref[i, 0] = cols_ref[i, 0]
        for t in range(1, 4):
            near_ref[i, t] = cols_ref[i, t] - 8
        for t in range(4, 12):
            p = cols_ref[i, t] - 40
            tile_ref[p] = 12 * i + t
            owner_block[p] = i
        return carry

    lax.fori_loop(0, 8, name, 0)

    def plane(k, carry):
        on = lax.rem(z - k + 8, 8)
        place = jnp.where(on == 0, 7, jnp.where(on == 4, 0, on - on // 5))
        i = owner_block[8 * k]
        slots_ref[i, 0] = 2 * place
        slots_ref[owner_block[8 * k + 7], 1] = 2 * place + 1
        for n in range(8):
            first_ref[8 * k + n] = jnp.where(owner_block[8 * k + n] == i, 1, 0)
        return carry

    lax.fori_loop(0, 8, plane, 0)


def tables(cols):
    return pl.pallas_call(
        table_kernel,
        out_shape=[
            jax.ShapeDtypeStruct(shape, jnp.int32) for shape in ((64,), (64,), (8, 4), (8, 2))
        ],
        in_specs=[sspec()],
        out_specs=[sspec()] * 4,
        scratch_shapes=[SMEM((64,), jnp.int32)],
    )(cols)


def publish_kernel(n, *refs):
    ins, outs, held, sems = refs[:n], refs[n : 2 * n], refs[2 * n : 3 * n], refs[3 * n]
    into = [pltpu.make_async_copy(i, h, sems.at[0, k]) for k, (i, h) in enumerate(zip(ins, held))]
    onto = [pltpu.make_async_copy(h, o, sems.at[1, k]) for k, (h, o) in enumerate(zip(held, outs))]
    for copy in into:
        copy.start()
    for first, then in zip(into, onto):
        first.wait()
        then.start()
    for copy in onto:
        copy.wait()


def published(*arrays):
    shapes = [jax.ShapeDtypeStruct(a.shape, a.dtype) for a in arrays]
    n = len(arrays)
    return pl.pallas_call(
        functools.partial(publish_kernel, n),
        out_shape=shapes,
        in_specs=[aspec()] * n,
        out_specs=[aspec()] * n,
        scratch_shapes=[VMEM(a.shape, a.dtype) for a in arrays] + [pltpu.SemaphoreType.DMA((2, n))],
        compiler_params=pltpu.CompilerParams(vmem_limit_bytes=63 * MIB),
        cost_estimate=cost(1e6, 6e6),
    )(*arrays)


def rem(a, n):
    return lax.rem(a + n, n)


def step_kernel(
    tile_ref, first_ref, cols_ref, from_ref, cnt_ref, pull_ref, weight_two_ref, weight_three_ref,
    hist_a_ref, hist_b_ref, tiles_hbm, prev_hbm, zero_hbm, grad_hbm,
    three_ref, fresh_ref, term_ref,
    *refs,
):
    refs = iter(refs)
    far, rows, same, other, partner, sums, s_mid, arrived = (
        [next(refs) for _ in range(3)] for _ in range(8)
    )
    (
        own_a, own_b, prev_ref, zero_ref, grad_ref, table, got, pack_ref, vin, idx_ref, idx_in,
        idx, tiles, home, second, low, three, share, share_c, share_xy, share_z, whole, v_mid,
        far_send, far_recv, y_send, y_recv, idx_send, idx_recv, v_send, v_recv,
        pair_send, pair_recv, sum_send, sum_recv, new_send, new_recv, local_sem,
        far_z_send, far_z_recv, gc_sem, gxy_send, gxy_recv, gz_send, gz_recv, hxy_send, hxy_recv,
    ) = refs
    z, x, core, turn = (lax.axis_index(a) for a in (Z, X, C, Y))
    hist = (hist_a_ref, hist_b_ref)
    own = (own_a, own_b)
    layer = (0, 1, 1)

    def remote(src, dst, send, recv, **to):
        return pltpu.make_async_remote_copy(
            src_ref=src, dst_ref=dst, send_sem=send, recv_sem=recv,
            device_id={AXES[a]: v for a, v in to.items()},
            device_id_type=pl.DeviceIdType.MESH,
        )

    barrier = pltpu.get_barrier_semaphore()

    def greet(**to):
        pl.semaphore_signal(
            barrier, inc=1, device_id={AXES[a]: v for a, v in to.items()},
            device_id_type=pl.DeviceIdType.MESH,
        )

    def greet_zc(o, carry):
        greet(z=rem(z + o // 2, 8), c=rem(core + o % 2, 2))
        greet(x=rem(x + o // 4, 4), y=rem(turn + o % 4, 4))
        return carry

    lax.fori_loop(1, 16, greet_zc, 0)

    local_copies = [
        pltpu.make_async_copy(hist[0], own_a, local_sem.at[0]),
        pltpu.make_async_copy(hist[1], own_b, local_sem.at[1]),
        pltpu.make_async_copy(prev_hbm, prev_ref, local_sem.at[3]),
        pltpu.make_async_copy(zero_hbm, zero_ref, local_sem.at[4]),
        pltpu.make_async_copy(grad_hbm, grad_ref, local_sem.at[7]),
    ]
    tiles_copy = pltpu.make_async_copy(tiles_hbm, tiles, local_sem.at[2])
    tiles_copy.start()

    def owner(g, d):
        return 8 * (g // 2) + 2 * lax.rem(x + d, 4) + lax.rem(g, 2)

    def want(g, carry):
        for d in range(4):
            p = owner(g, d)
            row = pull_ref[pl.ds(p, 1), :] + (4096 - 1024 * turn)
            idx_ref[g, d : d + 1, :] = lax.rem(row, 4096)
            idx_ref[g, 4 + d : 5 + d, :] = jnp.full((1, 128), first_ref[p], jnp.int32)
        return carry

    lax.fori_loop(0, 16, want, 0)

    lane = lax.broadcasted_iota(jnp.int32, (128, 128), 1)

    def pack(o):
        g = 2 * rem(z + o // 2, 8) + rem(core + o % 2, 2)
        for d in range(4):
            p = owner(g, d)
            tile = tiles[tile_ref[p]].astype(F32)
            tile = jnp.where(lane < cnt_ref[0, p], tile, 0.0).astype(BF)
            pack_ref[g, :, d * 128 : (d + 1) * 128] = tile

    size = 8 // PIECES
    down, up = rem(x + 3, 4), rem(x + 1, 4)

    def piece(l, d, q, h):
        return far[l].at[d, q, pl.ds(h * size, size)]

    def along_x(l, n, h):
        d, q, relayed, to = (
            (0, 0, None, down), (0, 1, None, down), (2, 1, None, up), (2, 0, None, up),
            (1, 0, (0, 0), down), (1, 1, (2, 1), up),
        )[n]
        if relayed is None:
            src = hist[layer[l]].at[pl.ds(rem(turn + q, 4) * 8 + h * size, size)]
            if l:
                src = src.at[:, :, pl.ds(128 * (l - 1), 128)]
        else:
            src = piece(l, *relayed, h)
        return remote(
            src, piece(l, d, q, h), far_send.at[l, n], far_recv.at[l, 2 * d + q, h], x=to
        )

    def along_y(l, d, q, h):
        to, at = (rem(turn + 1, 4), 3) if q == 0 else (rem(turn + 3, 4), 2)
        return remote(
            piece(l, d, q, h), piece(l, d, at, h),
            y_send.at[l, 2 * d + q], y_recv.at[l, 2 * d + q], y=to,
        )

    def x_here(l, d, q, h):
        remote(
            piece(l, d, q, h), piece(l, d, q, h),
            far_send.at[l, 0], far_recv.at[l, 2 * d + q, h], x=down,
        ).wait_recv()

    def whole_y(l, d, q):
        to, at = (rem(turn + 1, 4), 3) if q == 0 else (rem(turn + 3, 4), 2)
        return remote(
            far[l].at[d, q], far[l].at[d, at], y_send.at[l, 2 * d + q], y_recv.at[l, 2 * d + q], y=to
        )

    def whole_x(l, n):
        return remote(far[l].at[0, 0], far[l].at[0, 0], far_send.at[l, n], far_recv.at[l, 0, 0], x=up)

    def y_here(l, d):
        for q in range(2):
            whole_y(l, d, q).wait_recv()

    def own_rows(l):
        for n in (0, 2, 1, 3):
            for h in range(PIECES):
                along_x(l, n, h).start()

    def send_index(o):
        to_z, to_c = rem(z + o // 2, 8), rem(core + o % 2, 2)
        return remote(
            idx_ref.at[2 * to_z + to_c], idx_in.at[2 * z + core],
            idx_send.at[o], idx_recv.at[o], z=to_z, c=to_c,
        )

    def send_pack(o):
        to_z, to_c = rem(z + o // 2, 8), rem(core + o % 2, 2)
        return remote(
            pack_ref.at[2 * to_z + to_c], vin.at[2 * z + core],
            v_send.at[o], v_recv.at[o], z=to_z, c=to_c,
        )

    def pack_out(s):
        to_c = (core, 1 - core)[s]
        return remote(
            pack_ref.at[2 * rem(z + 4, 8) + to_c], v_mid.at[s],
            far_z_send.at[0, s], far_z_recv.at[0, s], z=rem(z + (1, 7)[s], 8),
        )

    def pack_on(s):
        source = rem(z + (7, 1)[s], 8)
        return remote(
            v_mid.at[s], vin.at[2 * source + core],
            v_send.at[8 + s], v_recv.at[8 + s], z=rem(source + 4, 8), c=(core, 1 - core)[s],
        )

    def sum_out(l, s):
        return remote(
            sums[l].at[s], s_mid[l].at[s],
            far_z_send.at[1 + l, s], far_z_recv.at[1 + l, s], z=rem(z + (1, 7)[s], 8),
        )

    def sum_on(l, s):
        return remote(
            s_mid[l].at[s], arrived[l].at[s],
            sum_send.at[l, 7 * s], sum_recv.at[l, 7 * s], z=rem(z + (3, 5)[s], 8),
        )

    def packs(act):
        each(2, 8, act)
        each(10, 16, act)
        act(1)

    def pass_packs():
        for s in range(2):
            pack_out(s).wait_recv()
            pack_on(s).start()

    def pass_sums(l):
        for s in range(2):
            sum_out(l, s).wait_recv()
            sum_on(l, s).start()

    def each(first, last, act):
        def body(o, carry):
            act(o)
            return carry

        lax.fori_loop(first, last, body, 0)

    pl.semaphore_wait(barrier, 30)
    own_rows(0)
    each(1, 16, lambda o: send_index(o).start())
    tiles_copy.wait()

    def pack_and_send(o):
        pack(o)
        send_pack(o - 1).start()

    pack(8)
    pack(9)
    pack_out(0).start()
    pack(10)
    pack_out(1).start()
    each(11, 16, pack_and_send)
    pack(1)
    send_pack(15).start()
    each(2, 8, pack_and_send)
    pack(0)
    send_pack(7).start()
    for copy in local_copies:
        copy.start()
    idx_in[2 * z + core] = idx_ref[2 * z + core]
    vin[2 * z + core] = pack_ref[2 * z + core]

    def gather(l, d):
        def widen(s, carry):
            r = pl.multiple_of(s * 128, 128)
            if d == 0:
                block = own[layer[l]][rem(s + 8 * turn, 32)]
                if l:
                    block = block[:, 128 * (l - 1) : 128 * l]
            else:
                block = far[l][d - 1, s // 8, lax.rem(s, 8)]
            block = block.astype(F32)
            if l:
                table[pl.ds(r, 128), :] = block
            else:
                table[pl.ds(2 * r, 128, stride=2), :] = block[:, :128]
                table[pl.ds(2 * r + 1, 128, stride=2), :] = block[:, 128:]
            return carry

        lax.fori_loop(0, 32, widen, 0)

        def worker(g):
            if l:
                for j in range(128):
                    got[pl.ds(j, 1), :] = table[pl.ds(idx[g, d, j], 1), :]
                both = got[0:128, :].astype(BF)
            else:
                for j in range(128):
                    got[pl.ds(2 * j, 2), :] = table[pl.ds(2 * idx[g, d, j], 2), :]
                left, right = got[pl.ds(0, 128, stride=2), :], got[pl.ds(1, 128, stride=2), :]
                both = jnp.concatenate([left, right], axis=1).astype(BF)
            rows[l][g, pl.ds(d * 128, 128), :] = both

        each(0, 16, worker)

    def away(n):
        return lax.rem(n + n // 4 + 4 * ((8 - n) // 8), 8)

    def product(l, n, which):
        g = rem(z + away(n), 8) * 2 + which
        packed = vin[g]
        flag = jnp.concatenate([idx_in[g, 4 + d : 5 + d, :] for d in range(4)], axis=1)
        flag = flag.astype(F32).astype(BF)
        both = jnp.concatenate([packed * flag, packed * (1 - flag)], axis=0)
        return jnp.dot(both, rows[l][g], preferred_element_type=F32)

    def to_partner(l, h):
        part = pl.ds(4 * h, 4)
        return remote(
            other[l].at[part], partner[l].at[part], pair_send.at[l, h], pair_recv.at[l, h],
            c=1 - core,
        )

    def send_sum(l, n):
        return remote(
            sums[l].at[pl.ds(2 * n, 2)], arrived[l].at[pl.ds(2 * n, 2)], sum_send.at[l, n], sum_recv.at[l, n],
            z=rem(z + away(n), 8),
        )

    def plane_sums(l):
        for h in range(2):
            def for_partner(n):
                other[l][n] = product(l, n, 1 - core).astype(BF)

            each(4 * h, 4 * h + 4, for_partner)
            if h:
                to_partner(l, 0).start()

        def for_me(n):
            same[l][n] = product(l, n, core)

        each(0, 4, for_me)
        to_partner(l, 1).start()
        each(4, 8, for_me)

        def add(n):
            both = (same[l][n] + partner[l][n].astype(F32)).astype(BF)
            sums[l][pl.ds(2 * n, 2)] = both.reshape(2, 128, both.shape[1])

        to_partner(l, 0).wait_recv()
        add(0)
        add(1)
        for s in range(2):
            sum_out(l, s).start()

        def add_and_send(n):
            add(n)
            send_sum(l, n - 1).start()

        each(2, 4, add_and_send)
        to_partner(l, 1).wait_recv()
        each(4, 8, add_and_send)

    def at_home(l):
        def block_sum(i):
            total = None
            for t in range(l, 4):
                b = cols_ref[i, t]
                block = own[l][b] if t else prev_ref[b]
                part = jnp.dot(tiles[12 * i + t], block, preferred_element_type=F32)
                total = part if total is None else total + part
            home[l, i] = total

        each(0, 8, block_sum)

    def finish(l, i):
        mine = pl.ds(pl.multiple_of(i * 128, 128), 128)
        parts = [
            arrived[st][from_ref[i, 0]].astype(F32) + arrived[st][from_ref[i, 1]].astype(F32)
            for st in range(3) if layer[st] == l
        ]
        total = home[l, i] + (parts[0] if l == 0 else jnp.concatenate(parts, axis=1))
        mixed = (1.0 - restart) * total + restart * zero_ref[mine, :].astype(F32)
        factor = math.log(strength / (l + 2) + 1.0)
        rounded = mixed.astype(BF)
        weight = (weight_two_ref, weight_three_ref)[l][...]
        out = jnp.dot(rounded, weight, preferred_element_type=F32)
        out = jnp.maximum((1.0 - factor) * mixed + factor * out, 0.0).astype(BF)
        return mine, rounded, out

    def relay(l):
        for h in range(PIECES):
            for n, d, q in ((4, 0, 0), (5, 2, 1)):
                x_here(l, d, q, h)
                along_x(l, n, h).start()
                along_y(l, d, q, h).start()

    def pass_on(l, *pairs):
        for h in range(PIECES):
            for d, q in pairs:
                x_here(l, d, q, h)
                along_y(l, d, q, h).start()

    def second_pair(l):
        pass_on(l, (2, 0), (0, 1))

    def third_pair(l):
        pass_on(l, (1, 0), (1, 1))

    def arrived_here(l):
        each(1, 7, lambda n: send_sum(l, n).wait_recv())
        for s in range(2):
            sum_on(l, s).wait_recv()

    for copy in local_copies:
        copy.wait()
    relay(0)
    own_rows(1)
    each(1, 16, lambda o: send_index(o).wait_recv())
    to_smem = pltpu.make_async_copy(idx_in, idx, local_sem.at[5])
    to_smem.start()
    to_smem.wait()
    gather(0, 0)
    at_home(0)
    pass_packs()
    second_pair(0)
    gather(1, 0)
    gather(2, 0)
    third_pair(0)
    y_here(0, 0)
    gather(0, 1)
    relay(1)
    own_rows(2)
    y_here(0, 2)
    gather(0, 3)
    second_pair(1)
    y_here(0, 1)
    gather(0, 2)
    packs(lambda o: send_pack(o).wait_recv())
    for s in range(2):
        pack_on(s).wait_recv()
    plane_sums(0)
    third_pair(1)
    at_home(1)
    relay(2)
    pass_sums(0)
    y_here(1, 0)
    gather(1, 1)
    y_here(1, 2)
    gather(1, 3)
    second_pair(2)
    y_here(1, 1)
    gather(1, 2)
    plane_sums(1)
    third_pair(2)
    y_here(2, 0)
    gather(2, 1)
    y_here(2, 2)
    gather(2, 3)
    pass_sums(1)
    y_here(2, 1)
    gather(2, 2)
    plane_sums(2)
    for st in range(3):
        arrived[st][14:16] = sums[st][14:16]
    arrived_here(0)

    def layer_two(i):
        second[i] = finish(0, i)[2]

    each(0, 8, layer_two)

    def add_current(i):
        block = second[cols_ref[i, 0]]
        home[1, i] += jnp.dot(tiles[12 * i], block, preferred_element_type=F32)

    each(0, 8, add_current)
    keep = pltpu.make_async_copy(second, fresh_ref.at[pl.ds(turn * 8, 8)], local_sem.at[6])
    keep.start()

    def new_rows(way, h, on):
        at = rem(turn + (0 if not on else (3, 1)[way]), 4) * 8 + 4 * h
        there = fresh_ref.at[pl.ds(at, 4)]
        here = there if on else second.at[pl.ds(4 * h, 4)]
        n = 3 * way + (2 if on else h)
        return remote(here, there, new_send.at[n], new_recv.at[n], y=rem(turn + (1, 3)[way], 4))

    def new_here(way, n):
        at = rem(turn + (2 if n == 2 else (3, 1)[way]), 4) * 8 + 4 * (way if n == 2 else n)
        half = fresh_ref.at[pl.ds(at, 4)]
        remote(
            half, half, new_send.at[3 * way], new_recv.at[3 * way + n], y=rem(turn + 1, 4)
        ).wait_recv()

    for h in range(2):
        for way in range(2):
            new_rows(way, (h, 1 - h)[way], False).start()
    pass_sums(2)
    for way in range(2):
        new_here(way, way)
        new_rows(way, way, True).start()
    arrived_here(1)
    arrived_here(2)

    def layer_three(i):
        mine, rounded, out = finish(1, i)
        three[mine, :] = out
        low[mine, :] = rounded

    each(0, 8, layer_three)
    three_copy = pltpu.make_async_copy(three, three_ref, local_sem.at[1])
    term = math.log(strength / 3 + 1.0) * lax.dot_general(
        low[...], grad_ref[...], (((0,), (0,)), ((), ())), preferred_element_type=F32
    )
    share[0:32] = term[:, :128].reshape(32, 8, 128)
    share[32:64] = term[:, 128:].reshape(32, 8, 128)
    three_copy.start()

    half, theirs = pl.ds(32 * core, 32), pl.ds(32 * (1 - core), 32)
    place = 2 * (4 * x + turn)

    def xy(o):
        return rem(x + o // 4, 4), rem(turn + o % 4, 4)

    def term_c():
        return remote(share.at[theirs], share_c, gc_sem.at[0], gc_sem.at[1], c=1 - core)

    def term_xy(o):
        to_x, to_y = xy(o)
        return remote(
            share_c.at[pl.ds(2 * (4 * to_x + to_y), 2)], share_xy.at[o],
            gxy_send.at[o], gxy_recv.at[o], x=to_x, y=to_y,
        )

    def term_z(dz):
        return remote(
            share_xy.at[0], share_z.at[z], gz_send.at[dz], gz_recv.at[dz], z=rem(z + dz, 8)
        )

    def back_xy(o):
        to_x, to_y = xy(o)
        mine = whole.at[pl.ds(32 * core + place, 2)]
        return remote(mine, mine, hxy_send.at[o], hxy_recv.at[o], x=to_x, y=to_y)

    def back_c():
        return remote(whole.at[half], whole.at[half], gc_sem.at[2], gc_sem.at[3], c=1 - core)

    term_c().start()
    term_c().wait_recv()
    share_c[...] = share_c[...] + share[half]
    each(1, 16, lambda o: term_xy(o).start())
    each(1, 16, lambda o: term_xy(o).wait_recv())
    total = share_c[pl.ds(place, 2)]
    for o in range(1, 16):
        total += share_xy[o]
    share_xy[0] = total
    share_z[z] = total
    each(1, 8, lambda o: term_z(o).start())
    each(1, 8, lambda o: term_z(o).wait_recv())
    total = share_z[0]
    for o in range(1, 8):
        total += share_z[o]
    whole[pl.ds(32 * core + place, 2)] = total
    each(1, 16, lambda o: back_xy(o).start())
    each(1, 16, lambda o: back_xy(o).wait_recv())
    back_c().start()
    back_c().wait_recv()
    term_ref[:, :128] = whole[0:32].reshape(256, 128)
    term_ref[:, 128:] = whole[32:64].reshape(256, 128)
    each(1, 16, lambda o: term_xy(o).wait_send())
    each(1, 8, lambda o: term_z(o).wait_send())
    each(1, 16, lambda o: back_xy(o).wait_send())
    three_copy.wait()
    term_c().wait_send()
    back_c().wait_send()
    for l in range(3):
        for n in range(6):
            whole_x(l, n).wait_send()
        for d in range(3):
            for q in range(2):
                whole_y(l, d, q).wait_send()
        for h in range(2):
            to_partner(l, h).wait_send()
        each(1, 7, lambda n: send_sum(l, n).wait_send())
        for s in range(2):
            sum_out(l, s).wait_send()
            sum_on(l, s).wait_send()
    each(1, 16, lambda o: send_index(o).wait_send())
    packs(lambda o: send_pack(o).wait_send())
    for s in range(2):
        pack_out(s).wait_send()
        pack_on(s).wait_send()
    keep.wait()
    for way in range(2):
        for n in (1 - way, 2):
            new_here(way, n)
        for h in range(2):
            new_rows(way, h, False).wait_send()
        new_rows(way, way, True).wait_send()


def whole_step(*args):
    dma = pltpu.SemaphoreType.DMA
    return pl.pallas_call(
        step_kernel,
        out_shape=(
            jax.ShapeDtypeStruct((1024, 256), BF),
            jax.ShapeDtypeStruct((32, 128, 256), BF),
            jax.ShapeDtypeStruct((256, 256), F32),
        ),
        in_specs=[sspec()] * 5 + [vspec()] * 3 + [aspec()] * 6,
        out_specs=(aspec(), aspec(), vspec()),
        scratch_shapes=[
            *(VMEM((3, 4, 8, 128, w), BF) for w in WIDTHS),
            *(VMEM((16, 512, w), BF) for w in WIDTHS),
            *(VMEM((8, 256, w), F32) for w in WIDTHS),
            *(VMEM((8, 256, w), BF) for w in WIDTHS),
            *(VMEM((8, 256, w), BF) for w in WIDTHS),
            *(VMEM((16, 128, w), BF) for w in WIDTHS),
            *(VMEM((2, 128, w), BF) for w in WIDTHS),
            *(VMEM((16, 128, w), BF) for w in WIDTHS),
            VMEM((32, 128, 256), BF),
            VMEM((32, 128, 256), BF),
            VMEM((8, 128, 256), BF),
            VMEM((1024, 256), BF),
            VMEM((1024, 256), BF),
            VMEM((8192, 128), F32),
            VMEM((256, 128), F32),
            VMEM((16, 128, 512), BF),
            VMEM((16, 128, 512), BF),
            VMEM((16, 8, 128), jnp.int32),
            VMEM((16, 8, 128), jnp.int32),
            SMEM((16, 8, 128), jnp.int32),
            VMEM((96, 128, 128), BF),
            VMEM((2, 8, 128, 256), F32),
            VMEM((8, 128, 256), BF),
            VMEM((1024, 256), BF),
            VMEM((1024, 256), BF),
            VMEM((64, 8, 128), F32),
            VMEM((32, 8, 128), F32),
            VMEM((16, 2, 8, 128), F32),
            VMEM((8, 2, 8, 128), F32),
            VMEM((64, 8, 128), F32),
            VMEM((2, 128, 512), BF),
            dma((3, 6)), dma((3, 6, PIECES)), dma((3, 6)), dma((3, 6)),
            dma((16,)), dma((16,)), dma((16,)), dma((16,)),
            dma((3, 2)), dma((3, 2)), dma((3, 8)), dma((3, 8)), dma((6,)), dma((6,)), dma((8,)),
            dma((4, 2)), dma((4, 2)), dma((4,)), dma((16,)), dma((16,)), dma((8,)), dma((8,)),
            dma((16,)), dma((16,)),
        ],
        compiler_params=pltpu.CompilerParams(
            vmem_limit_bytes=63 * MIB, collective_id=1, has_side_effects=True
        ),
        cost_estimate=cost(60e9, 40e6),
    )(*args)


def local(
    h_zero, h_prev, hist_a, hist_b, tile_vals, tile_cols, pull_rows, pull_counts,
    weight_two, weight_three, grad_out,
):
    tile_of, first, near, slots = tables(tile_cols)
    outs = whole_step(
        tile_of, first, near, slots, pull_counts, pull_rows.reshape(64, 128),
        weight_two, weight_three, hist_a.reshape(32, 128, 256), hist_b.reshape(32, 128, 256),
        tile_vals.reshape(96, 128, 128), h_prev.reshape(8, 128, 256), h_zero, grad_out,
    )
    layer_three, fresh_rows, grad_total = published(*outs)
    return (layer_three, fresh_rows.reshape(4096, 256), grad_total)


def solution(mesh):
    finer = Mesh(mesh.devices.reshape(8, 4, 2, mesh.shape["rep"]), (Z, X, C, Y))
    return jax.shard_map(
        local,
        mesh=finer,
        in_specs=(
            P(DEV_REP, None),
            P(DEV_REP, None),
            P(DEV, None),
            P(DEV, None),
            P(DEV_REP, None, None, None),
            P(DEV_REP, None),
            P(DEV_REP, None, None),
            P(DEV_REP, None),
            P(),
            P(),
            P(DEV_REP, None),
        ),
        out_specs=(P(DEV_REP, None), P(DEV, None), P()),
        check_vma=False,
    )
```
